32 devices in a mesh: cfg: 2 (over y), space: 8 (over z, x), tm: 2 (over core).
Axes of the slice: x: 2, y: 2, z: 4, core: 2. Of those that a mesh axis runs over, the one named last changes fastest.
Arguments:
- eigvecs: bfloat16 [4, 2304, 3, 2, 128], P(('cfg', 'tm'), 'space'), parts along dimension 0, may hold values from -6 to 6
- perambulator: bfloat16 [4, 8, 4, 2, 128, 128], P(('cfg', 'tm'), None, None, None, 'space'), parts along dimension 0, may hold values from -1 to 4
- momenta: int32 [1, 3], replicated, may hold values from 1 to 3
- source_slots: int32 [2], replicated, may hold values from 0 to 7, as said below
- gamma_columns: int32 [12, 4], replicated, may hold values from 0 to 3, each once within a row
- gamma_phases: int32 [12, 4], replicated, may hold values from 0 to 3
Outputs:
- meson: float32 [4, 128, 1, 12, 2, 128], P(('cfg', 'tm'), 'space'), parts along dimension 0
The draws below stay inside these ranges and needn't reach their ends.
There are 2 independent parts, one for each index of `cfg`. The reference program is written for one: setup_inputs(seed, part) draws one part's arguments, and reference() takes and returns one part's arrays. A program takes and returns all parts, laid end to end along the dimension named above; an argument that names none is the same for every part. Nothing has to cross between parts.
Inputs may be any that keep to these rules, and one draw needn't show every extreme that they name: `source_slots`: the two slots differ, and one of them is 7. `gamma_columns`: each row is a permutation of 0 to 3.
All inputs are finite; a program needn't handle non-finite values.
Results may differ from the reference program's by a relative error of at most 0.0049.
Values may be sent and summed in bfloat16 or wider, within the bound.
No kernel may reach another device: no remote copies, remote signals or barrier semaphores. Data moves between devices by JAX's collectives and lax.ppermute only.
A program may use at most 64 MiB of HBM per device.

```python
import math
import jax
import jax.numpy as jnp
from jax import lax

NEV = 128
NSTORE = 8
NMOM = 1
NGAM = 12
LY = 48
LZ = 48
NT = 2
SITES = 2304
LX = 1


def draw_perambulator(key, part):
    noise_key = jax.random.fold_in(key, 11)
    diag_key = jax.random.fold_in(key, 23)
    shape = (NT, NSTORE, 4, 2, NEV, NEV)
    noise = jax.random.normal(noise_key, shape, jnp.float32) * (0.6 / math.sqrt(NEV))
    diagonal = jnp.exp(jax.random.uniform(diag_key, (NT, NSTORE, 4, NEV), jnp.float32, -0.7, 0.7))
    identity = jnp.eye(NEV, dtype=jnp.float32)
    real_part = noise[:, :, :, 0] + diagonal[:, :, :, :, None] * identity
    return jnp.stack([real_part, noise[:, :, :, 1]], axis=3).astype(jnp.bfloat16)


def draw_source_slots(key, part):
    other_key = jax.random.fold_in(key, 31)
    order_key = jax.random.fold_in(key, 37)
    other = jax.random.randint(other_key, (), 0, NSTORE - 1, jnp.int32)
    last = jnp.full((), NSTORE - 1, jnp.int32)
    order = jax.random.randint(order_key, (), 0, 2, jnp.int32)
    first = jnp.where(order == 0, other, last)
    second = jnp.where(order == 0, last, other)
    return jnp.stack([first, second]).astype(jnp.int32)


def set_ends(result, own_key, low, high):
    longest = result.shape.index(max(result.shape))
    spots = []
    for shift in (0, 1):
        where = [jax.random.randint(jax.random.fold_in(own_key, axis), (), 0, length) for axis, length in enumerate(result.shape)]
        where[longest] = (where[longest] + shift) % result.shape[longest]
        spots.append(tuple(where))
    return result.at[spots[0]].set(low).at[spots[1]].set(high)


def with_spikes(entries, rng, source, target, blocks, factor):
    def block_of(dim):
        return (jnp.arange(entries.shape[dim]) // (entries.shape[dim] // blocks)).reshape((-1,) + (1,) * (entries.ndim - 1 - dim))

    near = jax.random.permutation(rng, blocks)[block_of(target)]
    other_side = (block_of(target) + blocks // 2) % blocks
    return jnp.where((block_of(source) == near) | (block_of(source) == other_side), factor * entries, entries)


def block_levels(own_key, dims, cuts, smallest, largest):
    def one(position, shards_of):
        draws = jax.random.uniform(jax.random.fold_in(jax.random.fold_in(own_key, 6), position), (shards_of,), jnp.float32, smallest / len(cuts), largest / len(cuts))
        return jnp.repeat(jnp.exp(draws), dims[position] // shards_of).reshape((-1,) + (1,) * (len(dims) - position - 1))

    level = one(*cuts[0])
    for cut in cuts[1:]:
        level = level * one(*cut)
    return level


def heavy_noise(key, shape, scale, reach, pieces, heavy, kind=jnp.bfloat16):
    drawn = scale * jax.random.normal(key, shape, jnp.float32)
    if pieces:
        drawn = drawn * block_levels(key, shape, pieces, -0.22, 0.18)
    return jnp.clip(with_spikes(drawn, jax.random.fold_in(key, 3), *heavy), -reach, reach).astype(kind)


def setup_inputs(seed: int = 0, part: int = 0) -> dict:
    key_of = jax.random.split(jax.random.key(seed), 7)
    part_keys = jax.random.split(jax.random.fold_in(key_of[6], part), 7)
    eigvecs = heavy_noise(part_keys[0], (NT, SITES, 3, 2, NEV), 1.0, 6.0, ((0, 2), (1, 8)), (1, 4, 8, 2.0))
    perambulator = draw_perambulator(jax.random.fold_in(jax.random.fold_in(key_of[6], part), 71), part)
    momenta = jax.random.randint(key_of[2], (NMOM, 3), 1, 4).astype(jnp.int32)
    source_slots = draw_source_slots(jax.random.fold_in(key_of[6], 71), part)
    gamma_columns = jax.vmap(lambda own: jax.random.permutation(own, 4))(jax.random.split(key_of[4], NGAM)).reshape((NGAM, 4)).astype(jnp.int32)
    gamma_phases = set_ends(jax.random.randint(key_of[5], (NGAM, 4), 0, 4), jax.random.fold_in(key_of[5], 1), 0, 3).astype(jnp.int32)
    return dict(eigvecs=eigvecs, perambulator=perambulator, momenta=momenta, source_slots=source_slots, gamma_columns=gamma_columns, gamma_phases=gamma_phases)


def gamma_mixer(gamma_columns, gamma_phases):
    spin_ids = jnp.arange(4, dtype=jnp.int32)
    matches = (gamma_columns[:, :, None] == spin_ids[None, None, :]).astype(jnp.float32)
    real_sign = (gamma_phases == 0).astype(jnp.float32) - (gamma_phases == 2).astype(jnp.float32)
    imag_sign = (gamma_phases == 1).astype(jnp.float32) - (gamma_phases == 3).astype(jnp.float32)
    real_part = matches * real_sign[:, :, None]
    imag_part = matches * imag_sign[:, :, None]
    first_row = jnp.stack([real_part, -imag_part], axis=-1)
    second_row = jnp.stack([imag_part, real_part], axis=-1)
    return jnp.stack([first_row, second_row], axis=1)

def apply_gammas(blocks, gamma_mix, factor):
    return factor * jnp.einsum('gostk,apstkb->apgob', gamma_mix, blocks, precision=lax.Precision.HIGHEST)

def phase_tables(momenta, site_ids, extent_x):
    coord_z = site_ids % LZ
    coord_y = site_ids // LZ % LY
    coord_x = site_ids // (LY * LZ)
    turns = (momenta[:, 0:1] * coord_x[None, :] % extent_x).astype(jnp.float32) / extent_x + (momenta[:, 1:2] * coord_y[None, :] % LY).astype(jnp.float32) / LY + (momenta[:, 2:3] * coord_z[None, :] % LZ).astype(jnp.float32) / LZ
    angles = 2.0 * math.pi * turns
    return (jnp.cos(angles), jnp.sin(angles))

def sink_vectors(vectors, picked):
    eig_count = picked.shape[-1]
    real_parts = []
    imag_parts = []
    for spin_index in range(4):
        real_tau = picked[spin_index, 0]
        imag_tau = picked[spin_index, 1]
        stacked = jnp.concatenate([jnp.concatenate([real_tau, imag_tau], axis=1), jnp.concatenate([-imag_tau, real_tau], axis=1)], axis=0)
        product = jnp.dot(vectors, stacked, preferred_element_type=jnp.float32).astype(jnp.bfloat16)
        real_parts.append(product[:, :eig_count])
        imag_parts.append(product[:, eig_count:])
    return (jnp.stack(real_parts, axis=1), jnp.stack(imag_parts, axis=1))

def twisted(right_real, right_imag, cosine, sine):
    moment_count, site_count = cosine.shape
    shaped_real = right_real.astype(jnp.float32).reshape(1, site_count, 3, 4, -1)
    shaped_imag = right_imag.astype(jnp.float32).reshape(1, site_count, 3, 4, -1)
    cosine_wide = cosine.reshape(moment_count, site_count, 1, 1, 1)
    sine_wide = sine.reshape(moment_count, site_count, 1, 1, 1)
    wave_real = (cosine_wide * shaped_real - sine_wide * shaped_imag).astype(jnp.bfloat16)
    wave_imag = (sine_wide * shaped_real + cosine_wide * shaped_imag).astype(jnp.bfloat16)
    return (wave_real.reshape(moment_count, site_count * 3, 4, -1), wave_imag.reshape(moment_count, site_count * 3, 4, -1))

def reference(eigvecs, perambulator, momenta, source_slots, gamma_columns, gamma_phases):
    factor = 1.0 / math.sqrt(12.0 * SITES)
    site_ids = jnp.arange(SITES, dtype=jnp.int32)
    cosine, sine = phase_tables(momenta, site_ids, LX)
    gamma_mix = gamma_mixer(gamma_columns, gamma_phases)
    chosen = jnp.take(perambulator, source_slots.astype(jnp.int32), axis=1)
    row_total = SITES * 3
    results = []
    for time_index in range(NT):
        vectors = eigvecs[time_index].reshape(row_total, 2 * NEV)
        left_real, left_imag = sink_vectors(vectors, chosen[time_index, 0])
        right_real, right_imag = sink_vectors(vectors, chosen[time_index, 1])
        wave_real, wave_imag = twisted(right_real, right_imag, cosine, sine)
        flat_left_real = left_real.reshape(row_total, 4 * NEV)
        flat_left_imag = left_imag.reshape(row_total, 4 * NEV)
        per_momentum = []
        for moment_index in range(NMOM):
            flat_wave_real = wave_real[moment_index].reshape(row_total, 4 * NEV)
            flat_wave_imag = wave_imag[moment_index].reshape(row_total, 4 * NEV)
            real_block = jnp.dot(flat_left_real.T, flat_wave_real, preferred_element_type=jnp.float32) + jnp.dot(flat_left_imag.T, flat_wave_imag, preferred_element_type=jnp.float32)
            imag_block = jnp.dot(flat_left_real.T, flat_wave_imag, preferred_element_type=jnp.float32) - jnp.dot(flat_left_imag.T, flat_wave_real, preferred_element_type=jnp.float32)
            both_parts = jnp.stack([real_block, imag_block], axis=0).reshape(2, 4, NEV, 4, NEV)
            per_momentum.append(both_parts.transpose(2, 1, 3, 0, 4))
        blocks = jnp.stack(per_momentum, axis=1)
        results.append(apply_gammas(blocks, gamma_mix, factor))
    return jnp.stack(results, axis=0)
```

```python
import functools
import math

import jax
import jax.numpy as jnp
from jax import lax
from jax.experimental import pallas as pl
from jax.experimental.pallas import tpu as pltpu
from jax.sharding import PartitionSpec as P

LY = 48
LZ = 48
SPINS = 4
COLORS = 3


def vmem():
    return pl.BlockSpec(memory_space=pltpu.VMEM)


def smem():
    return pl.BlockSpec(memory_space=pltpu.SMEM)


def dot(left, right, left_dim=1, right_dim=0):
    return lax.dot_general(
        left, right, (((left_dim,), (right_dim,)), ((), ())), preferred_element_type=jnp.float32
    )


def split(values):
    high = values.astype(jnp.bfloat16)
    return high, (values - high.astype(jnp.float32)).astype(jnp.bfloat16)


def wrapped(product, length):
    return product - length * jnp.floor(product * (1.0 / length) + 0.5 / length)


def pick_body(slots_ref, source_ref, out_ref):
    out_ref[...] = source_ref[...]


def pick_slots(perambulator, source_slots):
    block = (1, 1) + perambulator.shape[2:]
    zeros = (0,) * (len(block) - 2)
    return pl.pallas_call(
        pick_body,
        grid_spec=pltpu.PrefetchScalarGridSpec(
            num_scalar_prefetch=1,
            grid=(2,),
            in_specs=[pl.BlockSpec(block, lambda i, slots: (0, slots[i]) + zeros)],
            out_specs=pl.BlockSpec(block, lambda i, slots: (0, i) + zeros),
        ),
        out_shape=jax.ShapeDtypeStruct((1, 2) + perambulator.shape[2:], perambulator.dtype),
        name="pick_slots",
    )(source_slots, perambulator)


def overlap_body(extent_x, momentum_ref, vectors_ref, out_ref, wide_ref, left_ref, high_ref, low_ref):
    rows = left_ref.shape[0]
    eig = vectors_ref.shape[1]
    per_block = LZ * COLORS
    blocks = rows // per_block
    first_block = lax.axis_index("space") * blocks
    mom_x = momentum_ref[0].astype(jnp.float32)
    mom_y = momentum_ref[1].astype(jnp.float32)
    mom_z = momentum_ref[2].astype(jnp.float32)
    wide_ref[...] = vectors_ref[...].astype(jnp.float32)
    row_ids = lax.broadcasted_iota(jnp.int32, (per_block, eig), 0).astype(jnp.float32)
    coord_z = jnp.floor((row_ids + 0.5) * (1.0 / COLORS))
    angle_z = (2.0 * math.pi / LZ) * wrapped(mom_z * coord_z, LZ)
    cos_z = jnp.cos(angle_z)
    sin_z = jnp.sin(angle_z)
    padded = -(-blocks // 8) * 8
    block_ids = (lax.broadcasted_iota(jnp.int32, (padded, eig), 0) + first_block).astype(jnp.float32)
    coord_x = jnp.floor((block_ids + 0.5) * (1.0 / LY))
    coord_y = block_ids - LY * coord_x
    angle_b = 2.0 * math.pi * (
        wrapped(mom_x * coord_x, extent_x) / extent_x + wrapped(mom_y * coord_y, LY) / LY
    )
    cos_b = jnp.cos(angle_b)
    sin_b = jnp.sin(angle_b)
    for block in range(blocks):
        own = pl.ds(block * per_block, per_block)
        real = wide_ref[pl.ds(2 * block * per_block, per_block, stride=2), :]
        imag = wide_ref[pl.ds(2 * block * per_block + 1, per_block, stride=2), :]
        left_ref[own, :eig] = real.astype(jnp.bfloat16)
        left_ref[own, eig:] = imag.astype(jnp.bfloat16)
        cos_own = cos_b[block : block + 1, :]
        sin_own = sin_b[block : block + 1, :]
        cosine = cos_own * cos_z - sin_own * sin_z
        sine = sin_own * cos_z + cos_own * sin_z
        wave_real = cosine * real - sine * imag
        wave_imag = sine * real + cosine * imag
        for part, wave in ((0, wave_real), (1, wave_imag)):
            high, low = split(wave)
            lanes = slice(part * eig, (part + 1) * eig)
            high_ref[own, lanes] = high
            low_ref[own, lanes] = low
    left = left_ref[...]
    product = dot(left, high_ref[...], 0, 0) + dot(left, low_ref[...], 0, 0)
    out_ref[:, :eig] = product[:eig, :eig] + product[eig:, eig:]
    out_ref[:, eig:] = product[:eig, eig:] - product[eig:, :eig]


def overlap(rows_by_part, momentum, extent_x):
    rows = rows_by_part.shape[0] // 2
    eig = rows_by_part.shape[1]
    return pl.pallas_call(
        functools.partial(overlap_body, extent_x),
        in_specs=[smem(), vmem()],
        out_specs=vmem(),
        out_shape=jax.ShapeDtypeStruct((eig, 2 * eig), jnp.float32),
        scratch_shapes=[
            pltpu.VMEM((2 * rows, eig), jnp.float32),
            pltpu.VMEM((rows, 2 * eig), jnp.bfloat16),
            pltpu.VMEM((rows, 2 * eig), jnp.bfloat16),
            pltpu.VMEM((rows, 2 * eig), jnp.bfloat16),
        ],
        cost_estimate=pl.CostEstimate(
            flops=8 * rows * eig * eig * 2, bytes_accessed=4 * rows * eig, transcendentals=0
        ),
        name="overlap",
    )(momentum, rows_by_part)


def arrange_body(orders, *refs):
    pieces = refs[: len(orders)]
    left_ref, right_ref, full_ref = refs[len(orders) :]
    own = lax.axis_index("space")
    part_rows = pieces[0].shape[-2]
    eig = pieces[0].shape[-1]
    for piece, order in zip(pieces, orders):
        for index, relative in enumerate(order):
            start = pl.multiple_of((own ^ relative) * part_rows, part_rows)
            for spin in range(SPINS):
                for part in range(2):
                    full_ref[spin, part, pl.ds(start, part_rows), :] = piece[index, 0, spin, part]
                real = piece[index, 1, spin, 0]
                imag = piece[index, 1, spin, 1]
                right_ref[spin, pl.ds(start, part_rows), :eig] = real
                right_ref[spin, pl.ds(start, part_rows), eig:] = imag
                right_ref[spin, pl.ds(eig + start, part_rows), :eig] = -imag
                right_ref[spin, pl.ds(eig + start, part_rows), eig:] = real
    wanted = lax.broadcasted_iota(jnp.int32, (part_rows, eig), 0) + own * part_rows
    chosen = (lax.broadcasted_iota(jnp.int32, (part_rows, eig), 1) == wanted).astype(jnp.float32)
    chosen = chosen.astype(jnp.bfloat16)
    for spin in range(SPINS):
        for part in range(2):
            rows = dot(chosen, full_ref[spin, part], 1, 1).astype(jnp.bfloat16)
            left_ref[pl.ds(spin * part_rows, part_rows), part * eig : (part + 1) * eig] = rows


def arrange(pieces, orders):
    part_rows, eig = pieces[0].shape[-2:]
    return pl.pallas_call(
        functools.partial(arrange_body, orders),
        in_specs=[vmem()] * len(pieces),
        out_specs=[vmem(), vmem()],
        out_shape=[
            jax.ShapeDtypeStruct((SPINS * part_rows, 2 * eig), jnp.bfloat16),
            jax.ShapeDtypeStruct((SPINS, 2 * eig, 2 * eig), jnp.bfloat16),
        ],
        scratch_shapes=[pltpu.VMEM((SPINS, 2, eig, eig), jnp.bfloat16)],
        name="arrange",
    )(*pieces)


def finish_body(factor, columns_ref, phases_ref, mine_ref, theirs_ref, left_ref, right_ref, out_ref,
                high_ref, low_ref, blocks_ref):
    eig = mine_ref.shape[0]
    rows = out_ref.shape[0]
    total = (mine_ref[...] + theirs_ref[...]) * factor
    for part_ref, values in zip((high_ref, low_ref), split(total)):
        part_ref[:eig, :] = values
        part_ref[eig:, :eig] = values[:, eig:]
        part_ref[eig:, eig:] = -values[:, :eig]
    left = left_ref[...]
    front = dot(left, high_ref[...]) + dot(left, low_ref[...])
    high, low = split(front)
    both = jnp.concatenate([high, low], axis=0)
    for column in range(SPINS):
        product = dot(both, right_ref[column])
        product = product[: SPINS * rows] + product[SPINS * rows :]
        for spin in range(SPINS):
            for part in range(2):
                blocks_ref[column, spin, part] = product[
                    spin * rows : (spin + 1) * rows, part * eig : (part + 1) * eig
                ]
    for gamma in range(columns_ref.shape[0]):
        real = jnp.zeros((rows, eig), jnp.float32)
        imag = jnp.zeros((rows, eig), jnp.float32)
        for spin in range(SPINS):
            column = columns_ref[gamma, spin]
            phase = phases_ref[gamma, spin]
            along = (phase == 0).astype(jnp.float32) - (phase == 2).astype(jnp.float32)
            across = (phase == 1).astype(jnp.float32) - (phase == 3).astype(jnp.float32)
            block_real = blocks_ref[column, spin, 0]
            block_imag = blocks_ref[column, spin, 1]
            real = real + (along * block_real - across * block_imag)
            imag = imag + (across * block_real + along * block_imag)
        out_ref[:, 2 * gamma, :] = real
        out_ref[:, 2 * gamma + 1, :] = imag


def finish(mine, theirs, left, right, gamma_columns, gamma_phases, factor):
    eig = mine.shape[0]
    rows = left.shape[0] // SPINS
    gammas = gamma_columns.shape[0]
    return pl.pallas_call(
        functools.partial(finish_body, factor),
        in_specs=[smem(), smem(), vmem(), vmem(), vmem(), vmem()],
        out_specs=vmem(),
        out_shape=jax.ShapeDtypeStruct((rows, 2 * gammas, eig), jnp.float32),
        scratch_shapes=[
            pltpu.VMEM((2 * eig, 2 * eig), jnp.bfloat16),
            pltpu.VMEM((2 * eig, 2 * eig), jnp.bfloat16),
            pltpu.VMEM((SPINS, SPINS, 2, rows, eig), jnp.float32),
        ],
        name="finish",
    )(gamma_columns, gamma_phases, mine, theirs, left, right)


def finish_plain(total, chosen, gamma_columns, gamma_phases, factor):
    eig = total.shape[0]
    precise = functools.partial(jnp.einsum, precision=lax.Precision.HIGHEST)
    rows = eig // lax.axis_size("space")
    start = lax.axis_index("space") * rows
    left = lax.dynamic_slice_in_dim(chosen[0], start, rows, axis=3).astype(jnp.float32)
    right = chosen[1].astype(jnp.float32)
    real, imag = total[:, :eig], total[:, eig:]
    front_real = precise("sla,lm->sam", left[:, 0], real) + precise("sla,lm->sam", left[:, 1], imag)
    front_imag = precise("sla,lm->sam", left[:, 0], imag) - precise("sla,lm->sam", left[:, 1], real)
    block_real = precise("sam,tmb->astb", front_real, right[:, 0]) - precise(
        "sam,tmb->astb", front_imag, right[:, 1]
    )
    block_imag = precise("sam,tmb->astb", front_real, right[:, 1]) + precise(
        "sam,tmb->astb", front_imag, right[:, 0]
    )
    matches = (gamma_columns[:, :, None] == jnp.arange(SPINS)[None, None, :]).astype(jnp.float32)
    along = (gamma_phases == 0).astype(jnp.float32) - (gamma_phases == 2).astype(jnp.float32)
    across = (gamma_phases == 1).astype(jnp.float32) - (gamma_phases == 3).astype(jnp.float32)
    along = matches * along[:, :, None]
    across = matches * across[:, :, None]
    out_real = precise("gst,astb->agb", along, block_real) - precise("gst,astb->agb", across, block_imag)
    out_imag = precise("gst,astb->agb", across, block_real) + precise("gst,astb->agb", along, block_imag)
    return factor * jnp.stack([out_real, out_imag], axis=2).reshape(rows, -1, eig)


def swap(values, distance, ranks):
    return lax.ppermute(values, "space", [(rank, rank ^ distance) for rank in range(ranks)])


def on_device(eigvecs, perambulator, momenta, source_slots, gamma_columns, gamma_phases):
    local_sites = eigvecs.shape[1]
    eig_count = eigvecs.shape[4]
    ranks = lax.axis_size("space")
    total_sites = local_sites * ranks
    extent_x = total_sites // (LY * LZ)
    factor = 1.0 / math.sqrt(12.0 * total_sites)
    part_rows = perambulator.shape[4]
    rows_by_part = eigvecs.reshape(local_sites * COLORS * 2, eig_count)
    picked = pick_slots(perambulator, source_slots)
    tiled = ranks == 8 and part_rows % 16 == 0
    if tiled:
        pieces = [picked]
        orders = [(0,)]
        for distance in (4, 2, 1):
            held = pieces[0] if len(pieces) == 1 else jnp.concatenate(pieces, axis=0)
            order = tuple(relative for group in orders for relative in group)
            pieces.append(swap(held, distance, ranks))
            orders.append(tuple(relative ^ distance for relative in order))
        left, right = arrange(pieces, tuple(orders))
    else:
        chosen = lax.all_gather(picked[0], "space", axis=3, tiled=True)
    results = []
    for index in range(momenta.shape[0]):
        total = overlap(rows_by_part, momenta[index], extent_x)
        if tiled:
            total = total + swap(total, 1, ranks)
            total = total + swap(total, 2, ranks)
            rows = finish(total, swap(total, 4, ranks), left, right, gamma_columns, gamma_phases, factor)
        else:
            total = lax.psum(total, "space")
            rows = finish_plain(total, chosen, gamma_columns, gamma_phases, factor)
        results.append(rows.reshape(rows.shape[0], gamma_columns.shape[0], 2, eig_count))
    return jnp.stack(results, axis=1)[None]


def solution(mesh):
    in_specs = (
        P(("cfg", "tm"), "space", None, None, None),
        P(("cfg", "tm"), None, None, None, "space", None),
        P(),
        P(),
        P(),
        P(),
    )
    out_specs = P(("cfg", "tm"), "space", None, None, None, None)
    return jax.shard_map(
        on_device, mesh=mesh, in_specs=in_specs, out_specs=out_specs, check_vma=False
    )
```

```python
import functools
import math

import jax
import jax.numpy as jnp
from jax import lax
from jax.experimental import pallas as pl
from jax.experimental.pallas import tpu as pltpu
from jax.sharding import PartitionSpec as P

LY = 48
LZ = 48
SPINS = 4
COLORS = 3


def vmem():
    return pl.BlockSpec(memory_space=pltpu.VMEM)


def resident(array):
    return pltpu.with_memory_space_constraint(array, pltpu.VMEM)


def smem():
    return pl.BlockSpec(memory_space=pltpu.SMEM)


def dot(left, right, left_dim=1, right_dim=0):
    return lax.dot_general(
        left, right, (((left_dim,), (right_dim,)), ((), ())), preferred_element_type=jnp.float32
    )


def split(values):
    high = values.astype(jnp.bfloat16)
    return high, (values - high.astype(jnp.float32)).astype(jnp.bfloat16)


def wrapped(product, length):
    return product - length * jnp.floor(product * (1.0 / length) + 0.5 / length)


def pick_body(slots_ref, source_ref, out_ref, sems):
    copies = [
        pltpu.make_async_copy(source_ref.at[0, slots_ref[i]], out_ref.at[0, i], sems.at[i])
        for i in range(2)
    ]
    for copy in copies:
        copy.start()
    for copy in copies:
        copy.wait()


def pick_slots(perambulator, source_slots):
    return pl.pallas_call(
        pick_body,
        in_specs=[smem(), pl.BlockSpec(memory_space=pl.ANY)],
        out_specs=vmem(),
        out_shape=pltpu.VMEM((1, 2) + perambulator.shape[2:], perambulator.dtype),
        scratch_shapes=[pltpu.SemaphoreType.DMA((2,))],
        name="pick_slots",
    )(source_slots, perambulator)


def overlap_body(extent_x, momentum_ref, vectors_ref, out_ref, wide_ref, left_ref, high_ref, low_ref):
    rows = left_ref.shape[0]
    eig = vectors_ref.shape[1]
    per_block = LZ * COLORS
    blocks = rows // per_block
    first_block = lax.axis_index("space") * blocks
    mom_x = momentum_ref[0].astype(jnp.float32)
    mom_y = momentum_ref[1].astype(jnp.float32)
    mom_z = momentum_ref[2].astype(jnp.float32)
    wide_ref[...] = vectors_ref[...].astype(jnp.float32)
    row_ids = lax.broadcasted_iota(jnp.int32, (per_block, eig), 0).astype(jnp.float32)
    coord_z = jnp.floor((row_ids + 0.5) * (1.0 / COLORS))
    angle_z = (2.0 * math.pi / LZ) * wrapped(mom_z * coord_z, LZ)
    cos_z = jnp.cos(angle_z)
    sin_z = jnp.sin(angle_z)
    padded = -(-blocks // 8) * 8
    block_ids = (lax.broadcasted_iota(jnp.int32, (padded, eig), 0) + first_block).astype(jnp.float32)
    coord_x = jnp.floor((block_ids + 0.5) * (1.0 / LY))
    coord_y = block_ids - LY * coord_x
    angle_b = 2.0 * math.pi * (
        wrapped(mom_x * coord_x, extent_x) / extent_x + wrapped(mom_y * coord_y, LY) / LY
    )
    cos_b = jnp.cos(angle_b)
    sin_b = jnp.sin(angle_b)
    for block in range(blocks):
        own = pl.ds(block * per_block, per_block)
        real = wide_ref[pl.ds(2 * block * per_block, per_block, stride=2), :]
        imag = wide_ref[pl.ds(2 * block * per_block + 1, per_block, stride=2), :]
        left_ref[own, :eig] = real.astype(jnp.bfloat16)
        left_ref[own, eig:] = imag.astype(jnp.bfloat16)
        cos_own = cos_b[block : block + 1, :]
        sin_own = sin_b[block : block + 1, :]
        cosine = cos_own * cos_z - sin_own * sin_z
        sine = sin_own * cos_z + cos_own * sin_z
        wave_real = cosine * real - sine * imag
        wave_imag = sine * real + cosine * imag
        for part, wave in ((0, wave_real), (1, wave_imag)):
            high, low = split(wave)
            lanes = slice(part * eig, (part + 1) * eig)
            high_ref[own, lanes] = high
            low_ref[own, lanes] = low
    left = left_ref[...]
    product = dot(left, high_ref[...], 0, 0) + dot(left, low_ref[...], 0, 0)
    out_ref[:, :eig] = product[:eig, :eig] + product[eig:, eig:]
    out_ref[:, eig:] = product[:eig, eig:] - product[eig:, :eig]


def overlap(rows_by_part, momentum, extent_x):
    rows = rows_by_part.shape[0] // 2
    eig = rows_by_part.shape[1]
    return pl.pallas_call(
        functools.partial(overlap_body, extent_x),
        in_specs=[smem(), vmem()],
        out_specs=vmem(),
        out_shape=pltpu.VMEM((eig, 2 * eig), jnp.float32),
        scratch_shapes=[
            pltpu.VMEM((2 * rows, eig), jnp.float32),
            pltpu.VMEM((rows, 2 * eig), jnp.bfloat16),
            pltpu.VMEM((rows, 2 * eig), jnp.bfloat16),
            pltpu.VMEM((rows, 2 * eig), jnp.bfloat16),
        ],
        cost_estimate=pl.CostEstimate(
            flops=8 * rows * eig * eig * 2, bytes_accessed=4 * rows * eig, transcendentals=0
        ),
        name="overlap",
    )(momentum, rows_by_part)


def arrange_body(orders, *refs):
    pieces = refs[: len(orders)]
    left_ref, right_ref, full_ref = refs[len(orders) :]
    own = lax.axis_index("space")
    part_rows = pieces[0].shape[-2]
    eig = pieces[0].shape[-1]
    for piece, order in zip(pieces, orders):
        for index, relative in enumerate(order):
            start = pl.multiple_of((own ^ relative) * part_rows, part_rows)
            for spin in range(SPINS):
                for part in range(2):
                    full_ref[spin, part, pl.ds(start, part_rows), :] = piece[index, 0, spin, part]
                real = piece[index, 1, spin, 0]
                imag = piece[index, 1, spin, 1]
                right_ref[spin, pl.ds(start, part_rows), :eig] = real
                right_ref[spin, pl.ds(start, part_rows), eig:] = imag
                right_ref[spin, pl.ds(eig + start, part_rows), :eig] = -imag
                right_ref[spin, pl.ds(eig + start, part_rows), eig:] = real
    wanted = lax.broadcasted_iota(jnp.int32, (part_rows, eig), 0) + own * part_rows
    chosen = (lax.broadcasted_iota(jnp.int32, (part_rows, eig), 1) == wanted).astype(jnp.float32)
    chosen = chosen.astype(jnp.bfloat16)
    for spin in range(SPINS):
        for part in range(2):
            rows = dot(chosen, full_ref[spin, part], 1, 1).astype(jnp.bfloat16)
            left_ref[pl.ds(spin * part_rows, part_rows), part * eig : (part + 1) * eig] = rows


def arrange(pieces, orders):
    part_rows, eig = pieces[0].shape[-2:]
    return pl.pallas_call(
        functools.partial(arrange_body, orders),
        in_specs=[vmem()] * len(pieces),
        out_specs=[vmem(), vmem()],
        out_shape=[
            pltpu.VMEM((SPINS * part_rows, 2 * eig), jnp.bfloat16),
            pltpu.VMEM((SPINS, 2 * eig, 2 * eig), jnp.bfloat16),
        ],
        scratch_shapes=[pltpu.VMEM((SPINS, 2, eig, eig), jnp.bfloat16)],
        name="arrange",
    )(*[resident(piece) for piece in pieces])


def finish_body(factor, columns_ref, phases_ref, mine_ref, theirs_ref, left_ref, right_ref, out_ref,
                high_ref, low_ref, blocks_ref):
    eig = mine_ref.shape[0]
    rows = out_ref.shape[0]
    total = (mine_ref[...] + theirs_ref[...]) * factor
    for part_ref, values in zip((high_ref, low_ref), split(total)):
        part_ref[:eig, :] = values
        part_ref[eig:, :eig] = values[:, eig:]
        part_ref[eig:, eig:] = -values[:, :eig]
    left = left_ref[...]
    front = dot(left, high_ref[...]) + dot(left, low_ref[...])
    high, low = split(front)
    both = jnp.concatenate([high, low], axis=0)
    for column in range(SPINS):
        product = dot(both, right_ref[column])
        product = product[: SPINS * rows] + product[SPINS * rows :]
        for spin in range(SPINS):
            for part in range(2):
                blocks_ref[column, spin, part] = product[
                    spin * rows : (spin + 1) * rows, part * eig : (part + 1) * eig
                ]
    for gamma in range(columns_ref.shape[1]):
        real = jnp.zeros((rows, eig), jnp.float32)
        imag = jnp.zeros((rows, eig), jnp.float32)
        for spin in range(SPINS):
            column = columns_ref[spin, gamma]
            phase = phases_ref[spin, gamma]
            along = (phase == 0).astype(jnp.float32) - (phase == 2).astype(jnp.float32)
            across = (phase == 1).astype(jnp.float32) - (phase == 3).astype(jnp.float32)
            block_real = blocks_ref[column, spin, 0]
            block_imag = blocks_ref[column, spin, 1]
            real = real + (along * block_real - across * block_imag)
            imag = imag + (across * block_real + along * block_imag)
        out_ref[:, 2 * gamma, :] = real
        out_ref[:, 2 * gamma + 1, :] = imag


def finish(mine, theirs, left, right, gamma_columns, gamma_phases, factor):
    eig = mine.shape[0]
    rows = left.shape[0] // SPINS
    gammas = gamma_columns.shape[0]
    return pl.pallas_call(
        functools.partial(finish_body, factor),
        in_specs=[smem(), smem(), vmem(), vmem(), vmem(), vmem()],
        out_specs=vmem(),
        out_shape=jax.ShapeDtypeStruct((rows, 2 * gammas, eig), jnp.float32),
        scratch_shapes=[
            pltpu.VMEM((2 * eig, 2 * eig), jnp.bfloat16),
            pltpu.VMEM((2 * eig, 2 * eig), jnp.bfloat16),
            pltpu.VMEM((SPINS, SPINS, 2, rows, eig), jnp.float32),
        ],
        name="finish",
    )(
        gamma_columns.T, gamma_phases.T, resident(mine), resident(theirs), resident(left), resident(right)
    )


def finish_plain(total, chosen, gamma_columns, gamma_phases, factor):
    eig = total.shape[0]
    precise = functools.partial(jnp.einsum, precision=lax.Precision.HIGHEST)
    rows = eig // lax.axis_size("space")
    start = lax.axis_index("space") * rows
    left = lax.dynamic_slice_in_dim(chosen[0], start, rows, axis=3).astype(jnp.float32)
    right = chosen[1].astype(jnp.float32)
    real, imag = total[:, :eig], total[:, eig:]
    front_real = precise("sla,lm->sam", left[:, 0], real) + precise("sla,lm->sam", left[:, 1], imag)
    front_imag = precise("sla,lm->sam", left[:, 0], imag) - precise("sla,lm->sam", left[:, 1], real)
    block_real = precise("sam,tmb->astb", front_real, right[:, 0]) - precise(
        "sam,tmb->astb", front_imag, right[:, 1]
    )
    block_imag = precise("sam,tmb->astb", front_real, right[:, 1]) + precise(
        "sam,tmb->astb", front_imag, right[:, 0]
    )
    matches = (gamma_columns[:, :, None] == jnp.arange(SPINS)[None, None, :]).astype(jnp.float32)
    along = (gamma_phases == 0).astype(jnp.float32) - (gamma_phases == 2).astype(jnp.float32)
    across = (gamma_phases == 1).astype(jnp.float32) - (gamma_phases == 3).astype(jnp.float32)
    along = matches * along[:, :, None]
    across = matches * across[:, :, None]
    out_real = precise("gst,astb->agb", along, block_real) - precise("gst,astb->agb", across, block_imag)
    out_imag = precise("gst,astb->agb", across, block_real) + precise("gst,astb->agb", along, block_imag)
    return factor * jnp.stack([out_real, out_imag], axis=2).reshape(rows, -1, eig)


def swap(values, distance, ranks):
    return lax.ppermute(values, "space", [(rank, rank ^ distance) for rank in range(ranks)])


def on_device(eigvecs, perambulator, momenta, source_slots, gamma_columns, gamma_phases):
    local_sites = eigvecs.shape[1]
    eig_count = eigvecs.shape[4]
    ranks = lax.axis_size("space")
    total_sites = local_sites * ranks
    extent_x = total_sites // (LY * LZ)
    factor = 1.0 / math.sqrt(12.0 * total_sites)
    part_rows = perambulator.shape[4]
    rows_by_part = eigvecs.reshape(local_sites * COLORS * 2, eig_count)
    picked = pick_slots(perambulator, source_slots)
    tiled = ranks == 8 and part_rows % 16 == 0
    if tiled:
        pieces = [picked]
        orders = [(0,)]
        for distance in (4, 2, 1):
            held = pieces[0] if len(pieces) == 1 else jnp.concatenate(pieces, axis=0)
            order = tuple(relative for group in orders for relative in group)
            pieces.append(swap(held, distance, ranks))
            orders.append(tuple(relative ^ distance for relative in order))
        left, right = arrange(pieces, tuple(orders))
    else:
        chosen = lax.all_gather(picked[0], "space", axis=3, tiled=True)
    results = []
    for index in range(momenta.shape[0]):
        total = overlap(rows_by_part, momenta[index], extent_x)
        if tiled:
            total = total + swap(total, 1, ranks)
            total = total + swap(total, 2, ranks)
            rows = finish(total, swap(total, 4, ranks), left, right, gamma_columns, gamma_phases, factor)
        else:
            total = lax.psum(total, "space")
            rows = finish_plain(total, chosen, gamma_columns, gamma_phases, factor)
        results.append(rows.reshape(rows.shape[0], gamma_columns.shape[0], 2, eig_count))
    return jnp.stack(results, axis=1)[None]


def solution(mesh):
    in_specs = (
        P(("cfg", "tm"), "space", None, None, None),
        P(("cfg", "tm"), None, None, None, "space", None),
        P(),
        P(),
        P(),
        P(),
    )
    out_specs = P(("cfg", "tm"), "space", None, None, None, None)
    return jax.shard_map(
        on_device, mesh=mesh, in_specs=in_specs, out_specs=out_specs, check_vma=False
    )
```

```python
import functools
import math

import jax
import jax.numpy as jnp
from jax import lax
from jax.experimental import pallas as pl
from jax.experimental.pallas import tpu as pltpu
from jax.sharding import PartitionSpec as P

LY = 48
LZ = 48
SPINS = 4
COLORS = 3


def vmem():
    return pl.BlockSpec(memory_space=pltpu.VMEM)


def resident(array):
    return pltpu.with_memory_space_constraint(array, pltpu.VMEM)


def scalars(array):
    return pltpu.with_memory_space_constraint(array, pltpu.SMEM)


def smem():
    return pl.BlockSpec(memory_space=pltpu.SMEM)


def dot(left, right, left_dim=1, right_dim=0):
    return lax.dot_general(
        left, right, (((left_dim,), (right_dim,)), ((), ())), preferred_element_type=jnp.float32
    )


def split(values):
    high = values.astype(jnp.bfloat16)
    return high, (values - high.astype(jnp.float32)).astype(jnp.bfloat16)


def wrapped(product, length):
    return product - length * jnp.floor(product * (1.0 / length) + 0.5 / length)


def load_body(slots_ref, source_ref, vectors_ref, picked_ref, loaded_ref, sems):
    copies = [pltpu.make_async_copy(vectors_ref, loaded_ref, sems.at[2])]
    copies += [
        pltpu.make_async_copy(source_ref.at[0, slots_ref[i]], picked_ref.at[0, i], sems.at[i])
        for i in range(2)
    ]
    for copy in copies:
        copy.start()
    for copy in copies:
        copy.wait()


def load(perambulator, source_slots, rows_by_part):
    return pl.pallas_call(
        load_body,
        in_specs=[smem(), pl.BlockSpec(memory_space=pl.ANY), pl.BlockSpec(memory_space=pl.ANY)],
        out_specs=[vmem(), vmem()],
        out_shape=[
            pltpu.VMEM((1, 2) + perambulator.shape[2:], perambulator.dtype),
            pltpu.VMEM(rows_by_part.shape, rows_by_part.dtype),
        ],
        scratch_shapes=[pltpu.SemaphoreType.DMA((3,))],
        name="load",
    )(source_slots, perambulator, rows_by_part)


def overlap_body(extent_x, momentum_ref, vectors_ref, out_ref, narrow_ref, wide_ref, left_ref, high_ref, low_ref):
    rows = left_ref.shape[0]
    eig = vectors_ref.shape[1]
    per_block = LZ * COLORS
    blocks = rows // per_block
    first_block = lax.axis_index("space") * blocks
    mom_x = momentum_ref[0].astype(jnp.float32)
    mom_y = momentum_ref[1].astype(jnp.float32)
    mom_z = momentum_ref[2].astype(jnp.float32)
    wide_ref[...] = vectors_ref[...].astype(jnp.float32)
    row_ids = lax.broadcasted_iota(jnp.int32, (per_block, eig), 0).astype(jnp.float32)
    coord_z = jnp.floor((row_ids + 0.5) * (1.0 / COLORS))
    angle_z = (2.0 * math.pi / LZ) * wrapped(mom_z * coord_z, LZ)
    cos_z = jnp.cos(angle_z)
    sin_z = jnp.sin(angle_z)
    padded = -(-blocks // 8) * 8
    block_ids = (lax.broadcasted_iota(jnp.int32, (padded, eig), 0) + first_block).astype(jnp.float32)
    coord_x = jnp.floor((block_ids + 0.5) * (1.0 / LY))
    coord_y = block_ids - LY * coord_x
    angle_b = 2.0 * math.pi * (
        wrapped(mom_x * coord_x, extent_x) / extent_x + wrapped(mom_y * coord_y, LY) / LY
    )
    cos_b = jnp.cos(angle_b)
    sin_b = jnp.sin(angle_b)
    for block in range(blocks):
        own = pl.ds(block * per_block, per_block)
        real = wide_ref[pl.ds(2 * block * per_block, per_block, stride=2), :]
        imag = wide_ref[pl.ds(2 * block * per_block + 1, per_block, stride=2), :]
        left_ref[own, :eig] = real.astype(jnp.bfloat16)
        left_ref[own, eig:] = imag.astype(jnp.bfloat16)
        cos_own = cos_b[block : block + 1, :]
        sin_own = sin_b[block : block + 1, :]
        cosine = cos_own * cos_z - sin_own * sin_z
        sine = sin_own * cos_z + cos_own * sin_z
        wave_real = cosine * real - sine * imag
        wave_imag = sine * real + cosine * imag
        for part, wave in ((0, wave_real), (1, wave_imag)):
            high, low = split(wave)
            lanes = slice(part * eig, (part + 1) * eig)
            high_ref[own, lanes] = high
            low_ref[own, lanes] = low
    left = left_ref[...]
    product = dot(left, high_ref[...], 0, 0) + dot(left, low_ref[...], 0, 0)
    out_ref[:, :eig] = product[:eig, :eig] + product[eig:, eig:]
    out_ref[:, eig:] = product[:eig, eig:] - product[eig:, :eig]
    narrow_ref[...] = out_ref[...].astype(jnp.bfloat16)


def overlap(rows_by_part, momentum, extent_x):
    rows = rows_by_part.shape[0] // 2
    eig = rows_by_part.shape[1]
    return pl.pallas_call(
        functools.partial(overlap_body, extent_x),
        in_specs=[smem(), vmem()],
        out_specs=[vmem(), vmem()],
        out_shape=[
            pltpu.VMEM((eig, 2 * eig), jnp.float32),
            pltpu.VMEM((eig, 2 * eig), jnp.bfloat16),
        ],
        scratch_shapes=[
            pltpu.VMEM((2 * rows, eig), jnp.float32),
            pltpu.VMEM((rows, 2 * eig), jnp.bfloat16),
            pltpu.VMEM((rows, 2 * eig), jnp.bfloat16),
            pltpu.VMEM((rows, 2 * eig), jnp.bfloat16),
        ],
        cost_estimate=pl.CostEstimate(
            flops=8 * rows * eig * eig * 2, bytes_accessed=4 * rows * eig, transcendentals=0
        ),
        name="overlap",
    )(scalars(momentum), resident(rows_by_part))


def arrange_body(orders, *refs):
    pieces = refs[: len(orders)]
    left_ref, right_ref, full_ref = refs[len(orders) :]
    own = lax.axis_index("space")
    part_rows = pieces[0].shape[-2]
    eig = pieces[0].shape[-1]
    for piece, order in zip(pieces, orders):
        for index, relative in enumerate(order):
            start = pl.multiple_of((own ^ relative) * part_rows, part_rows)
            for spin in range(SPINS):
                for part in range(2):
                    full_ref[spin, part, pl.ds(start, part_rows), :] = piece[index, 0, spin, part]
                real = piece[index, 1, spin, 0]
                imag = piece[index, 1, spin, 1]
                right_ref[spin, pl.ds(start, part_rows), :eig] = real
                right_ref[spin, pl.ds(start, part_rows), eig:] = imag
                right_ref[spin, pl.ds(eig + start, part_rows), :eig] = -imag
                right_ref[spin, pl.ds(eig + start, part_rows), eig:] = real
    wanted = lax.broadcasted_iota(jnp.int32, (part_rows, eig), 0) + own * part_rows
    chosen = (lax.broadcasted_iota(jnp.int32, (part_rows, eig), 1) == wanted).astype(jnp.float32)
    chosen = chosen.astype(jnp.bfloat16)
    for spin in range(SPINS):
        for part in range(2):
            rows = dot(chosen, full_ref[spin, part], 1, 1).astype(jnp.bfloat16)
            left_ref[pl.ds(spin * part_rows, part_rows), part * eig : (part + 1) * eig] = rows


def arrange(pieces, orders):
    part_rows, eig = pieces[0].shape[-2:]
    return pl.pallas_call(
        functools.partial(arrange_body, orders),
        in_specs=[vmem()] * len(pieces),
        out_specs=[vmem(), vmem()],
        out_shape=[
            pltpu.VMEM((SPINS * part_rows, 2 * eig), jnp.bfloat16),
            pltpu.VMEM((SPINS, 2 * eig, 2 * eig), jnp.bfloat16),
        ],
        scratch_shapes=[pltpu.VMEM((SPINS, 2, eig, eig), jnp.bfloat16)],
        name="arrange",
    )(*[resident(piece) for piece in pieces])


def finish_body(factor, columns_ref, phases_ref, mine_ref, theirs_ref, left_ref, right_ref, out_ref,
                high_ref, low_ref, blocks_ref):
    eig = mine_ref.shape[0]
    rows = out_ref.shape[0]
    total = (mine_ref[...] + theirs_ref[...].astype(jnp.float32)) * factor
    for part_ref, values in zip((high_ref, low_ref), split(total)):
        part_ref[:eig, :] = values
        part_ref[eig:, :eig] = values[:, eig:]
        part_ref[eig:, eig:] = -values[:, :eig]
    left = left_ref[...]
    front = dot(left, high_ref[...]) + dot(left, low_ref[...])
    high, low = split(front)
    both = jnp.concatenate([high, low], axis=0)
    for column in range(SPINS):
        product = dot(both, right_ref[column])
        product = product[: SPINS * rows] + product[SPINS * rows :]
        for spin in range(SPINS):
            for part in range(2):
                blocks_ref[column, spin, part] = product[
                    spin * rows : (spin + 1) * rows, part * eig : (part + 1) * eig
                ]
    for gamma in range(columns_ref.shape[1]):
        real = jnp.zeros((rows, eig), jnp.float32)
        imag = jnp.zeros((rows, eig), jnp.float32)
        for spin in range(SPINS):
            column = columns_ref[spin, gamma]
            phase = phases_ref[spin, gamma]
            along = (phase == 0).astype(jnp.float32) - (phase == 2).astype(jnp.float32)
            across = (phase == 1).astype(jnp.float32) - (phase == 3).astype(jnp.float32)
            block_real = blocks_ref[column, spin, 0]
            block_imag = blocks_ref[column, spin, 1]
            real = real + (along * block_real - across * block_imag)
            imag = imag + (across * block_real + along * block_imag)
        out_ref[:, 2 * gamma, :] = real
        out_ref[:, 2 * gamma + 1, :] = imag


def finish(mine, theirs, left, right, gamma_columns, gamma_phases, factor):
    eig = mine.shape[0]
    rows = left.shape[0] // SPINS
    gammas = gamma_columns.shape[0]
    return pl.pallas_call(
        functools.partial(finish_body, factor),
        in_specs=[smem(), smem(), vmem(), vmem(), vmem(), vmem()],
        out_specs=vmem(),
        out_shape=jax.ShapeDtypeStruct((rows, 2 * gammas, eig), jnp.float32),
        scratch_shapes=[
            pltpu.VMEM((2 * eig, 2 * eig), jnp.bfloat16),
            pltpu.VMEM((2 * eig, 2 * eig), jnp.bfloat16),
            pltpu.VMEM((SPINS, SPINS, 2, rows, eig), jnp.float32),
        ],
        name="finish",
    )(
        scalars(gamma_columns.T), scalars(gamma_phases.T), resident(mine), resident(theirs), resident(left), resident(right)
    )


def finish_plain(total, chosen, gamma_columns, gamma_phases, factor):
    eig = total.shape[0]
    precise = functools.partial(jnp.einsum, precision=lax.Precision.HIGHEST)
    rows = eig // lax.axis_size("space")
    start = lax.axis_index("space") * rows
    left = lax.dynamic_slice_in_dim(chosen[0], start, rows, axis=3).astype(jnp.float32)
    right = chosen[1].astype(jnp.float32)
    real, imag = total[:, :eig], total[:, eig:]
    front_real = precise("sla,lm->sam", left[:, 0], real) + precise("sla,lm->sam", left[:, 1], imag)
    front_imag = precise("sla,lm->sam", left[:, 0], imag) - precise("sla,lm->sam", left[:, 1], real)
    block_real = precise("sam,tmb->astb", front_real, right[:, 0]) - precise(
        "sam,tmb->astb", front_imag, right[:, 1]
    )
    block_imag = precise("sam,tmb->astb", front_real, right[:, 1]) + precise(
        "sam,tmb->astb", front_imag, right[:, 0]
    )
    matches = (gamma_columns[:, :, None] == jnp.arange(SPINS)[None, None, :]).astype(jnp.float32)
    along = (gamma_phases == 0).astype(jnp.float32) - (gamma_phases == 2).astype(jnp.float32)
    across = (gamma_phases == 1).astype(jnp.float32) - (gamma_phases == 3).astype(jnp.float32)
    along = matches * along[:, :, None]
    across = matches * across[:, :, None]
    out_real = precise("gst,astb->agb", along, block_real) - precise("gst,astb->agb", across, block_imag)
    out_imag = precise("gst,astb->agb", across, block_real) + precise("gst,astb->agb", along, block_imag)
    return factor * jnp.stack([out_real, out_imag], axis=2).reshape(rows, -1, eig)


def swap(values, distance, ranks):
    return lax.ppermute(values, "space", [(rank, rank ^ distance) for rank in range(ranks)])


def on_device(eigvecs, perambulator, momenta, source_slots, gamma_columns, gamma_phases):
    local_sites = eigvecs.shape[1]
    eig_count = eigvecs.shape[4]
    ranks = lax.axis_size("space")
    total_sites = local_sites * ranks
    extent_x = total_sites // (LY * LZ)
    factor = 1.0 / math.sqrt(12.0 * total_sites)
    part_rows = perambulator.shape[4]
    rows_by_part = eigvecs.reshape(local_sites * COLORS * 2, eig_count)
    picked, rows_by_part = load(perambulator, source_slots, rows_by_part)
    tiled = ranks == 8 and part_rows % 16 == 0
    if tiled:
        pieces = [picked]
        orders = [(0,)]
        for distance in (4, 2, 1):
            held = pieces[0] if len(pieces) == 1 else jnp.concatenate(pieces, axis=0)
            order = tuple(relative for group in orders for relative in group)
            pieces.append(swap(held, distance, ranks))
            orders.append(tuple(relative ^ distance for relative in order))
        left, right = arrange(pieces, tuple(orders))
    else:
        chosen = lax.all_gather(picked[0], "space", axis=3, tiled=True)
    results = []
    for index in range(momenta.shape[0]):
        total, narrow = overlap(rows_by_part, momenta[index], extent_x)
        if tiled:
            for distance in (1, 2):
                received = swap(narrow, distance, ranks)
                total = total + received.astype(jnp.float32)
                narrow = total.astype(jnp.bfloat16)
            received = swap(narrow, 4, ranks)
            rows = finish(total, received, left, right, gamma_columns, gamma_phases, factor)
        else:
            total = lax.psum(total, "space")
            rows = finish_plain(total, chosen, gamma_columns, gamma_phases, factor)
        results.append(rows.reshape(rows.shape[0], gamma_columns.shape[0], 2, eig_count))
    return jnp.stack(results, axis=1)[None]


def solution(mesh):
    in_specs = (
        P(("cfg", "tm"), "space", None, None, None),
        P(("cfg", "tm"), None, None, None, "space", None),
        P(),
        P(),
        P(),
        P(),
    )
    out_specs = P(("cfg", "tm"), "space", None, None, None, None)
    return jax.shard_map(
        on_device, mesh=mesh, in_specs=in_specs, out_specs=out_specs, check_vma=False
    )
```

```python
import functools
import math

import jax
import jax.numpy as jnp
from jax import lax
from jax.experimental import pallas as pl
from jax.experimental.pallas import tpu as pltpu
from jax.sharding import PartitionSpec as P

LY = 48
LZ = 48
SPINS = 4
COLORS = 3
SLOT_DISTANCES = (1, 4, 2)
SUM_DISTANCES = (2, 1, 4)
KEPT_OWNERS = [e for e in range(8) if not e & SLOT_DISTANCES[0]]
SENT_OWNERS = [e for e in range(8) if e & SLOT_DISTANCES[0]]


def vmem():
    return pl.BlockSpec(memory_space=pltpu.VMEM)


def resident(array):
    return pltpu.with_memory_space_constraint(array, pltpu.VMEM)


def scalars(array):
    return pltpu.with_memory_space_constraint(array, pltpu.SMEM)


def smem():
    return pl.BlockSpec(memory_space=pltpu.SMEM)


def dot(left, right, left_dim=1, right_dim=0):
    return lax.dot_general(
        left, right, (((left_dim,), (right_dim,)), ((), ())), preferred_element_type=jnp.float32
    )


def split(values):
    high = values.astype(jnp.bfloat16)
    return high, (values - high.astype(jnp.float32)).astype(jnp.bfloat16)


def wrapped(product, length):
    return product - length * jnp.floor(product * (1.0 / length) + 0.5 / length)


def load_body(slots_ref, source_ref, vectors_ref, sent_ref, kept_ref, loaded_ref, first_ref, turned_ref, sems):
    pairs = SPINS * 2
    part_rows, eig = source_ref.shape[-2:]
    kept = kept_ref.shape[0]
    copies = [
        pltpu.make_async_copy(source_ref.at[0, slots_ref[0]], first_ref, sems.at[0]),
        pltpu.make_async_copy(source_ref.at[0, slots_ref[1]], sent_ref.at[pl.ds(0, pairs)], sems.at[1]),
        pltpu.make_async_copy(vectors_ref, loaded_ref, sems.at[2]),
    ]
    for copy in copies:
        copy.start()
    copies[0].wait()
    own = lax.axis_index("space")
    turned_ref[...] = first_ref[...].reshape(pairs * part_rows, eig).T
    for relative in range(2 * kept):
        start = pl.multiple_of((own ^ relative) * part_rows, part_rows)
        block = turned_ref[pl.ds(start, part_rows), :]
        if relative in KEPT_OWNERS:
            kept_ref[KEPT_OWNERS.index(relative)] = block
        else:
            sent_ref[pairs + SENT_OWNERS.index(relative)] = block
    copies[1].wait()
    copies[2].wait()


def load(perambulator, source_slots, rows_by_part):
    _, slots, spins, parts, part_rows, eig = perambulator.shape
    pairs = spins * parts
    kept = eig // part_rows // 2
    kind = perambulator.dtype
    return pl.pallas_call(
        load_body,
        in_specs=[smem(), pl.BlockSpec(memory_space=pl.ANY), pl.BlockSpec(memory_space=pl.ANY)],
        out_specs=[vmem(), vmem(), vmem()],
        out_shape=[
            pltpu.VMEM((pairs + kept, part_rows, eig), kind),
            pltpu.VMEM((kept, part_rows, eig), kind),
            pltpu.VMEM(rows_by_part.shape, rows_by_part.dtype),
        ],
        scratch_shapes=[
            pltpu.VMEM((pairs, part_rows, eig), kind),
            pltpu.VMEM((eig, pairs * part_rows), kind),
            pltpu.SemaphoreType.DMA((3,)),
        ],
        name="load",
    )(source_slots, perambulator.reshape(1, slots, pairs, part_rows, eig), rows_by_part)


def overlap_body(extent_x, momentum_ref, vectors_ref, out_ref, narrow_ref, wide_ref, left_ref, high_ref, low_ref):
    rows = left_ref.shape[0]
    eig = vectors_ref.shape[1]
    per_block = LZ * COLORS
    blocks = rows // per_block
    first_block = lax.axis_index("space") * blocks
    mom_x = momentum_ref[0].astype(jnp.float32)
    mom_y = momentum_ref[1].astype(jnp.float32)
    mom_z = momentum_ref[2].astype(jnp.float32)
    wide_ref[...] = vectors_ref[...].astype(jnp.float32)
    row_ids = lax.broadcasted_iota(jnp.int32, (per_block, eig), 0).astype(jnp.float32)
    coord_z = jnp.floor((row_ids + 0.5) * (1.0 / COLORS))
    angle_z = (2.0 * math.pi / LZ) * wrapped(mom_z * coord_z, LZ)
    cos_z = jnp.cos(angle_z)
    sin_z = jnp.sin(angle_z)
    padded = -(-blocks // 8) * 8
    block_ids = (lax.broadcasted_iota(jnp.int32, (padded, eig), 0) + first_block).astype(jnp.float32)
    coord_x = jnp.floor((block_ids + 0.5) * (1.0 / LY))
    coord_y = block_ids - LY * coord_x
    angle_b = 2.0 * math.pi * (
        wrapped(mom_x * coord_x, extent_x) / extent_x + wrapped(mom_y * coord_y, LY) / LY
    )
    cos_b = jnp.cos(angle_b)
    sin_b = jnp.sin(angle_b)
    for block in range(blocks):
        own = pl.ds(block * per_block, per_block)
        real = wide_ref[pl.ds(2 * block * per_block, per_block, stride=2), :]
        imag = wide_ref[pl.ds(2 * block * per_block + 1, per_block, stride=2), :]
        left_ref[own, :eig] = real.astype(jnp.bfloat16)
        left_ref[own, eig:] = imag.astype(jnp.bfloat16)
        cos_own = cos_b[block : block + 1, :]
        sin_own = sin_b[block : block + 1, :]
        cosine = cos_own * cos_z - sin_own * sin_z
        sine = sin_own * cos_z + cos_own * sin_z
        wave_real = cosine * real - sine * imag
        wave_imag = sine * real + cosine * imag
        for part, wave in ((0, wave_real), (1, wave_imag)):
            high, low = split(wave)
            lanes = slice(part * eig, (part + 1) * eig)
            high_ref[own, lanes] = high
            low_ref[own, lanes] = low
    left = left_ref[...]
    product = dot(left, high_ref[...], 0, 0) + dot(left, low_ref[...], 0, 0)
    out_ref[:, :eig] = product[:eig, :eig] + product[eig:, eig:]
    out_ref[:, eig:] = product[:eig, eig:] - product[eig:, :eig]
    narrow_ref[...] = out_ref[...].astype(jnp.bfloat16)


def overlap(rows_by_part, momentum, extent_x):
    rows = rows_by_part.shape[0] // 2
    eig = rows_by_part.shape[1]
    return pl.pallas_call(
        functools.partial(overlap_body, extent_x),
        in_specs=[smem(), vmem()],
        out_specs=[vmem(), vmem()],
        out_shape=[
            pltpu.VMEM((eig, 2 * eig), jnp.float32),
            pltpu.VMEM((eig, 2 * eig), jnp.bfloat16),
        ],
        scratch_shapes=[
            pltpu.VMEM((2 * rows, eig), jnp.float32),
            pltpu.VMEM((rows, 2 * eig), jnp.bfloat16),
            pltpu.VMEM((rows, 2 * eig), jnp.bfloat16),
            pltpu.VMEM((rows, 2 * eig), jnp.bfloat16),
        ],
        cost_estimate=pl.CostEstimate(
            flops=8 * rows * eig * eig * 2, bytes_accessed=4 * rows * eig, transcendentals=0
        ),
        name="overlap",
    )(scalars(momentum), resident(rows_by_part))


def arrange_body(plan, *refs):
    pieces = refs[:-2]
    left_ref, right_ref = refs[-2:]
    pairs = SPINS * 2
    own = lax.axis_index("space")
    part_rows, eig = pieces[0].shape[1:]
    lane_groups = lax.broadcasted_iota(jnp.int32, (part_rows, eig), 1) // part_rows
    rows = [jnp.zeros((part_rows, eig), jnp.float32) for _ in range(pairs)]
    for relative, right_piece, right_start, left_piece, left_index in plan:
        group = own ^ relative
        start = pl.multiple_of(group * part_rows, part_rows)
        for spin in range(SPINS):
            real = pieces[right_piece][right_start + 2 * spin]
            imag = pieces[right_piece][right_start + 2 * spin + 1]
            right_ref[spin, pl.ds(start, part_rows), :eig] = real
            right_ref[spin, pl.ds(start, part_rows), eig:] = imag
            right_ref[spin, pl.ds(eig + start, part_rows), :eig] = -imag
            right_ref[spin, pl.ds(eig + start, part_rows), eig:] = real
        block = pieces[left_piece][left_index].astype(jnp.float32)
        inside = lane_groups == group
        for pair in range(pairs):
            shift = lax.rem((group - pair + pairs) * part_rows, eig)
            rows[pair] = jnp.where(inside, pltpu.roll(block, shift, 1), rows[pair])
    for pair in range(pairs):
        spin, part = pair // 2, pair % 2
        left_ref[pl.ds(spin * part_rows, part_rows), part * eig : (part + 1) * eig] = rows[pair].astype(
            jnp.bfloat16
        )


def arrange(pieces, plan):
    part_rows, eig = pieces[0].shape[1:]
    return pl.pallas_call(
        functools.partial(arrange_body, plan),
        in_specs=[vmem()] * len(pieces),
        out_specs=[vmem(), vmem()],
        out_shape=[
            pltpu.VMEM((SPINS * part_rows, 2 * eig), jnp.bfloat16),
            pltpu.VMEM((SPINS, 2 * eig, 2 * eig), jnp.bfloat16),
        ],
        name="arrange",
    )(*[resident(piece) for piece in pieces])


def finish_body(factor, columns_ref, phases_ref, mine_ref, theirs_ref, left_ref, right_ref, out_ref,
                high_ref, low_ref, blocks_ref):
    eig = mine_ref.shape[0]
    rows = out_ref.shape[0]
    total = (mine_ref[...] + theirs_ref[...].astype(jnp.float32)) * factor
    for part_ref, values in zip((high_ref, low_ref), split(total)):
        part_ref[:eig, :] = values
        part_ref[eig:, :eig] = values[:, eig:]
        part_ref[eig:, eig:] = -values[:, :eig]
    left = left_ref[...]
    front = dot(left, high_ref[...]) + dot(left, low_ref[...])
    high, low = split(front)
    both = jnp.concatenate([high, low], axis=0)
    for column in range(SPINS):
        product = dot(both, right_ref[column])
        product = product[: SPINS * rows] + product[SPINS * rows :]
        for spin in range(SPINS):
            for part in range(2):
                blocks_ref[column, spin, part] = product[
                    spin * rows : (spin + 1) * rows, part * eig : (part + 1) * eig
                ]
    for gamma in range(columns_ref.shape[1]):
        real = jnp.zeros((rows, eig), jnp.float32)
        imag = jnp.zeros((rows, eig), jnp.float32)
        for spin in range(SPINS):
            column = columns_ref[spin, gamma]
            phase = phases_ref[spin, gamma]
            along = (phase == 0).astype(jnp.float32) - (phase == 2).astype(jnp.float32)
            across = (phase == 1).astype(jnp.float32) - (phase == 3).astype(jnp.float32)
            block_real = blocks_ref[column, spin, 0]
            block_imag = blocks_ref[column, spin, 1]
            real = real + (along * block_real - across * block_imag)
            imag = imag + (across * block_real + along * block_imag)
        out_ref[:, 2 * gamma, :] = real
        out_ref[:, 2 * gamma + 1, :] = imag


def finish(mine, theirs, left, right, gamma_columns, gamma_phases, factor):
    eig = mine.shape[0]
    rows = left.shape[0] // SPINS
    gammas = gamma_columns.shape[0]
    return pl.pallas_call(
        functools.partial(finish_body, factor),
        in_specs=[smem(), smem(), vmem(), vmem(), vmem(), vmem()],
        out_specs=vmem(),
        out_shape=jax.ShapeDtypeStruct((rows, 2 * gammas, eig), jnp.float32),
        scratch_shapes=[
            pltpu.VMEM((2 * eig, 2 * eig), jnp.bfloat16),
            pltpu.VMEM((2 * eig, 2 * eig), jnp.bfloat16),
            pltpu.VMEM((SPINS, SPINS, 2, rows, eig), jnp.float32),
        ],
        name="finish",
    )(
        scalars(gamma_columns.T), scalars(gamma_phases.T), resident(mine), resident(theirs), resident(left), resident(right)
    )


def finish_plain(total, chosen, gamma_columns, gamma_phases, factor):
    eig = total.shape[0]
    precise = functools.partial(jnp.einsum, precision=lax.Precision.HIGHEST)
    rows = eig // lax.axis_size("space")
    start = lax.axis_index("space") * rows
    left = lax.dynamic_slice_in_dim(chosen[0], start, rows, axis=3).astype(jnp.float32)
    right = chosen[1].astype(jnp.float32)
    real, imag = total[:, :eig], total[:, eig:]
    front_real = precise("sla,lm->sam", left[:, 0], real) + precise("sla,lm->sam", left[:, 1], imag)
    front_imag = precise("sla,lm->sam", left[:, 0], imag) - precise("sla,lm->sam", left[:, 1], real)
    block_real = precise("sam,tmb->astb", front_real, right[:, 0]) - precise(
        "sam,tmb->astb", front_imag, right[:, 1]
    )
    block_imag = precise("sam,tmb->astb", front_real, right[:, 1]) + precise(
        "sam,tmb->astb", front_imag, right[:, 0]
    )
    matches = (gamma_columns[:, :, None] == jnp.arange(SPINS)[None, None, :]).astype(jnp.float32)
    along = (gamma_phases == 0).astype(jnp.float32) - (gamma_phases == 2).astype(jnp.float32)
    across = (gamma_phases == 1).astype(jnp.float32) - (gamma_phases == 3).astype(jnp.float32)
    along = matches * along[:, :, None]
    across = matches * across[:, :, None]
    out_real = precise("gst,astb->agb", along, block_real) - precise("gst,astb->agb", across, block_imag)
    out_imag = precise("gst,astb->agb", across, block_real) + precise("gst,astb->agb", along, block_imag)
    return factor * jnp.stack([out_real, out_imag], axis=2).reshape(rows, -1, eig)


def swap(values, distance, ranks):
    return lax.ppermute(values, "space", [(rank, rank ^ distance) for rank in range(ranks)])


def gather_slots(perambulator, source_slots, rows_by_part, ranks):
    pairs = SPINS * 2
    sent, kept, rows_by_part = load(perambulator, source_slots, rows_by_part)
    pieces = [sent, kept]
    shards = [(0, 0, 0)]
    columns = {(0, relative): (1, index) for index, relative in enumerate(KEPT_OWNERS)}
    for distance in SLOT_DISTANCES:
        if distance == SLOT_DISTANCES[0]:
            held = sent
            moved = [(0, relative) for relative in SENT_OWNERS]
        else:
            moved = [key for key in columns if key[1] & distance]
            held = jnp.concatenate(
                [pieces[piece][first : first + pairs] for _, piece, first in shards]
                + [pieces[piece][index][None] for piece, index in (columns.pop(key) for key in moved)],
                axis=0,
            )
        pieces.append(swap(held, distance, ranks))
        arrived = len(pieces) - 1
        shards += [
            (source ^ distance, arrived, pairs * count) for count, (source, _, _) in enumerate(shards)
        ]
        for count, (source, owner) in enumerate(moved):
            columns[(source ^ distance, owner ^ distance)] = (arrived, pairs * len(shards) // 2 + count)
    plan = tuple(
        (source, piece, first) + columns[(source, 0)] for source, piece, first in shards
    )
    left, right = arrange(pieces, plan)
    return left, right, rows_by_part


def on_device(eigvecs, perambulator, momenta, source_slots, gamma_columns, gamma_phases):
    local_sites = eigvecs.shape[1]
    eig_count = eigvecs.shape[4]
    ranks = lax.axis_size("space")
    total_sites = local_sites * ranks
    extent_x = total_sites // (LY * LZ)
    factor = 1.0 / math.sqrt(12.0 * total_sites)
    part_rows = perambulator.shape[4]
    rows_by_part = eigvecs.reshape(local_sites * COLORS * 2, eig_count)
    tiled = ranks == 8 and part_rows % 16 == 0 and part_rows * ranks == eig_count
    if tiled:
        left, right, rows_by_part = gather_slots(perambulator, source_slots, rows_by_part, ranks)
    else:
        chosen = lax.all_gather(
            jnp.take(perambulator[0], source_slots, axis=0), "space", axis=3, tiled=True
        )
    results = []
    for index in range(momenta.shape[0]):
        total, narrow = overlap(rows_by_part, momenta[index], extent_x)
        if tiled:
            for distance in SUM_DISTANCES[:2]:
                received = swap(narrow, distance, ranks)
                total = total + received.astype(jnp.float32)
                narrow = total.astype(jnp.bfloat16)
            received = swap(narrow, SUM_DISTANCES[2], ranks)
            rows = finish(total, received, left, right, gamma_columns, gamma_phases, factor)
        else:
            total = lax.psum(total, "space")
            rows = finish_plain(total, chosen, gamma_columns, gamma_phases, factor)
        results.append(rows.reshape(rows.shape[0], gamma_columns.shape[0], 2, eig_count))
    return jnp.stack(results, axis=1)[None]


def solution(mesh):
    in_specs = (
        P(("cfg", "tm"), "space", None, None, None),
        P(("cfg", "tm"), None, None, None, "space", None),
        P(),
        P(),
        P(),
        P(),
    )
    out_specs = P(("cfg", "tm"), "space", None, None, None, None)
    return jax.shard_map(
        on_device, mesh=mesh, in_specs=in_specs, out_specs=out_specs, check_vma=False
    )
```

```python
import functools
import math

import jax
import jax.numpy as jnp
from jax import lax
from jax.experimental import pallas as pl
from jax.experimental.pallas import tpu as pltpu
from jax.sharding import PartitionSpec as P

LY = 48
LZ = 48
SPINS = 4
COLORS = 3
TURNS = 5
SLOT_DISTANCES = (1, 4, 2)
SUM_DISTANCES = (2, 1, 4)
KEPT_OWNERS = [e for e in range(8) if not e & SLOT_DISTANCES[0]]
SENT_OWNERS = [e for e in range(8) if e & SLOT_DISTANCES[0]]


def vmem():
    return pl.BlockSpec(memory_space=pltpu.VMEM)


def resident(array):
    return pltpu.with_memory_space_constraint(array, pltpu.VMEM)


def scalars(array):
    return pltpu.with_memory_space_constraint(array, pltpu.SMEM)


def smem():
    return pl.BlockSpec(memory_space=pltpu.SMEM)


def dot(left, right, left_dim=1, right_dim=0):
    return lax.dot_general(
        left, right, (((left_dim,), (right_dim,)), ((), ())), preferred_element_type=jnp.float32
    )


def split(values):
    high = values.astype(jnp.bfloat16)
    return high, (values - high.astype(jnp.float32)).astype(jnp.bfloat16)


def wrapped(product, length):
    return product - length * jnp.floor(product * (1.0 / length) + 0.5 / length)


def load_body(slots_hbm, momenta_hbm, columns_hbm, phases_hbm, source_ref, vectors_ref,
              sent_ref, kept_ref, loaded_ref, numbers_ref,
              stored_ref, turned_ref, slots_ref, momenta_ref, columns_ref, phases_ref, sems):
    pairs = SPINS * 2
    part_rows, eig = source_ref.shape[-2:]
    kept = kept_ref.shape[0]
    copies = [
        pltpu.make_async_copy(slots_hbm, slots_ref, sems.at[0]),
        pltpu.make_async_copy(source_ref.at[0], stored_ref, sems.at[1]),
        pltpu.make_async_copy(vectors_ref, loaded_ref, sems.at[2]),
        pltpu.make_async_copy(momenta_hbm, momenta_ref, sems.at[3]),
        pltpu.make_async_copy(columns_hbm, columns_ref, sems.at[4]),
        pltpu.make_async_copy(phases_hbm, phases_ref, sems.at[5]),
    ]
    for copy in copies:
        copy.start()
    copies[0].wait()
    copies[1].wait()
    sent_ref[pl.ds(0, pairs)] = stored_ref[slots_ref[1]]
    own = lax.axis_index("space")
    turned_ref[...] = stored_ref[slots_ref[0]].reshape(pairs * part_rows, eig).T
    for relative in range(2 * kept):
        start = pl.multiple_of((own ^ relative) * part_rows, part_rows)
        block = turned_ref[pl.ds(start, part_rows), :]
        if relative in KEPT_OWNERS:
            kept_ref[KEPT_OWNERS.index(relative)] = block
        else:
            sent_ref[pairs + SENT_OWNERS.index(relative)] = block
    for copy in copies[3:]:
        copy.wait()
    count, axes = momenta_ref.shape
    for index in range(count):
        for axis in range(axes):
            numbers_ref[index * axes + axis] = momenta_ref[index, axis]
    for gamma in range(columns_ref.shape[1]):
        for spin in range(SPINS):
            place = (columns_ref[spin, gamma] * SPINS + spin) * TURNS + phases_ref[spin, gamma]
            numbers_ref[count * axes + gamma * SPINS + spin] = place
    copies[2].wait()


def load(perambulator, source_slots, rows_by_part, momenta, gamma_columns, gamma_phases):
    _, slots, spins, parts, part_rows, eig = perambulator.shape
    pairs = spins * parts
    kept = eig // part_rows // 2
    kind = perambulator.dtype
    return pl.pallas_call(
        load_body,
        in_specs=[pl.BlockSpec(memory_space=pl.ANY)] * 6,
        out_specs=[vmem(), vmem(), vmem(), smem()],
        out_shape=[
            pltpu.VMEM((pairs + kept, part_rows, eig), kind),
            pltpu.VMEM((kept, part_rows, eig), kind),
            pltpu.VMEM(rows_by_part.shape, rows_by_part.dtype),
            pltpu.SMEM((momenta.size + gamma_columns.size,), jnp.int32),
        ],
        scratch_shapes=[
            pltpu.VMEM((slots, pairs, part_rows, eig), kind),
            pltpu.VMEM((eig, pairs * part_rows), kind),
            pltpu.SMEM(source_slots.shape, jnp.int32),
            pltpu.SMEM(momenta.shape, jnp.int32),
            pltpu.SMEM(gamma_columns.shape[::-1], jnp.int32),
            pltpu.SMEM(gamma_phases.shape[::-1], jnp.int32),
            pltpu.SemaphoreType.DMA((6,)),
        ],
        name="load",
    )(
        source_slots,
        momenta,
        gamma_columns.T,
        gamma_phases.T,
        perambulator.reshape(1, slots, pairs, part_rows, eig),
        rows_by_part,
    )


def overlap_body(extent_x, first, numbers_ref, vectors_ref, out_ref, narrow_ref, wide_ref, left_ref, both_ref):
    rows = left_ref.shape[0]
    eig = vectors_ref.shape[1]
    per_block = LZ * COLORS
    blocks = rows // per_block
    first_block = lax.axis_index("space") * blocks
    mom_x = numbers_ref[first + 0].astype(jnp.float32)
    mom_y = numbers_ref[first + 1].astype(jnp.float32)
    mom_z = numbers_ref[first + 2].astype(jnp.float32)
    wide_ref[...] = vectors_ref[...].astype(jnp.float32)
    row_ids = lax.broadcasted_iota(jnp.int32, (per_block, eig), 0).astype(jnp.float32)
    coord_z = jnp.floor((row_ids + 0.5) * (1.0 / COLORS))
    angle_z = (2.0 * math.pi / LZ) * wrapped(mom_z * coord_z, LZ)
    cos_z = jnp.cos(angle_z)
    sin_z = jnp.sin(angle_z)
    padded = -(-blocks // 8) * 8
    block_ids = (lax.broadcasted_iota(jnp.int32, (padded, eig), 0) + first_block).astype(jnp.float32)
    coord_x = jnp.floor((block_ids + 0.5) * (1.0 / LY))
    coord_y = block_ids - LY * coord_x
    angle_b = 2.0 * math.pi * (
        wrapped(mom_x * coord_x, extent_x) / extent_x + wrapped(mom_y * coord_y, LY) / LY
    )
    cos_b = jnp.cos(angle_b)
    sin_b = jnp.sin(angle_b)
    for block in range(blocks):
        own = pl.ds(block * per_block, per_block)
        real = wide_ref[pl.ds(2 * block * per_block, per_block, stride=2), :]
        imag = wide_ref[pl.ds(2 * block * per_block + 1, per_block, stride=2), :]
        left_ref[own, :eig] = real.astype(jnp.bfloat16)
        left_ref[own, eig:] = imag.astype(jnp.bfloat16)
        cos_own = cos_b[block : block + 1, :]
        sin_own = sin_b[block : block + 1, :]
        cosine = cos_own * cos_z - sin_own * sin_z
        sine = sin_own * cos_z + cos_own * sin_z
        wave_real = cosine * real - sine * imag
        wave_imag = sine * real + cosine * imag
        for part, wave in ((0, wave_real), (1, wave_imag)):
            high, low = split(wave)
            lanes = slice(part * eig, (part + 1) * eig)
            both_ref[own, lanes] = high
            both_ref[own, slice(lanes.start + 2 * eig, lanes.stop + 2 * eig)] = low
    left = left_ref[...]
    product = dot(left, both_ref[...], 0, 0)
    product = product[:, : 2 * eig] + product[:, 2 * eig :]
    out_ref[:, :eig] = product[:eig, :eig] + product[eig:, eig:]
    out_ref[:, eig:] = product[:eig, eig:] - product[eig:, :eig]
    narrow_ref[...] = out_ref[...].astype(jnp.bfloat16)


def overlap(rows_by_part, numbers, index, extent_x):
    rows = rows_by_part.shape[0] // 2
    eig = rows_by_part.shape[1]
    return pl.pallas_call(
        functools.partial(overlap_body, extent_x, 3 * index),
        in_specs=[smem(), vmem()],
        out_specs=[vmem(), vmem()],
        out_shape=[
            pltpu.VMEM((eig, 2 * eig), jnp.float32),
            pltpu.VMEM((eig, 2 * eig), jnp.bfloat16),
        ],
        scratch_shapes=[
            pltpu.VMEM((2 * rows, eig), jnp.float32),
            pltpu.VMEM((rows, 2 * eig), jnp.bfloat16),
            pltpu.VMEM((rows, 4 * eig), jnp.bfloat16),
        ],
        cost_estimate=pl.CostEstimate(
            flops=8 * rows * eig * eig * 2, bytes_accessed=4 * rows * eig, transcendentals=0
        ),
        name="overlap",
    )(scalars(numbers), resident(rows_by_part))


def arrange_body(plan, *refs):
    pieces = refs[:-2]
    left_ref, right_ref = refs[-2:]
    pairs = SPINS * 2
    own = lax.axis_index("space")
    part_rows, eig = pieces[0].shape[1:]
    lane_groups = lax.broadcasted_iota(jnp.int32, (part_rows, eig), 1) // part_rows
    rows = [jnp.zeros((part_rows, eig), jnp.float32) for _ in range(pairs)]
    for relative, right_piece, right_start, left_piece, left_index in plan:
        group = own ^ relative
        start = pl.multiple_of(group * part_rows, part_rows)
        for spin in range(SPINS):
            real = pieces[right_piece][right_start + 2 * spin]
            imag = pieces[right_piece][right_start + 2 * spin + 1]
            right_ref[spin, pl.ds(start, part_rows), :eig] = real
            right_ref[spin, pl.ds(start, part_rows), eig:] = imag
            right_ref[spin, pl.ds(eig + start, part_rows), :eig] = -imag
            right_ref[spin, pl.ds(eig + start, part_rows), eig:] = real
        block = pieces[left_piece][left_index].astype(jnp.float32)
        inside = lane_groups == group
        for pair in range(pairs):
            shift = lax.rem((group - pair + pairs) * part_rows, eig)
            rows[pair] = jnp.where(inside, pltpu.roll(block, shift, 1), rows[pair])
    for pair in range(pairs):
        spin, part = pair // 2, pair % 2
        left_ref[pl.ds(spin * part_rows, part_rows), part * eig : (part + 1) * eig] = rows[pair].astype(
            jnp.bfloat16
        )


def arrange(pieces, plan):
    part_rows, eig = pieces[0].shape[1:]
    return pl.pallas_call(
        functools.partial(arrange_body, plan),
        in_specs=[vmem()] * len(pieces),
        out_specs=[vmem(), vmem()],
        out_shape=[
            pltpu.VMEM((SPINS * part_rows, 2 * eig), jnp.bfloat16),
            pltpu.VMEM((SPINS, 2 * eig, 2 * eig), jnp.bfloat16),
        ],
        name="arrange",
    )(*[resident(piece) for piece in pieces])


def finish_body(factor, first, numbers_ref, mine_ref, theirs_ref, left_ref, right_ref, out_ref,
                high_ref, low_ref, blocks_ref):
    eig = mine_ref.shape[0]
    rows = out_ref.shape[0]
    total = (mine_ref[...] + theirs_ref[...].astype(jnp.float32)) * factor
    for part_ref, values in zip((high_ref, low_ref), split(total)):
        part_ref[:eig, :] = values
        part_ref[eig:, :eig] = values[:, eig:]
        part_ref[eig:, eig:] = -values[:, :eig]
    left = left_ref[...]
    front = dot(left, high_ref[...]) + dot(left, low_ref[...])
    high, low = split(front)
    both = jnp.concatenate([high, low], axis=0)
    for column in range(SPINS):
        product = dot(both, right_ref[column])
        product = product[: SPINS * rows] + product[SPINS * rows :]
        for spin in range(SPINS):
            real = product[spin * rows : (spin + 1) * rows, :eig]
            imag = product[spin * rows : (spin + 1) * rows, eig:]
            start = (column * SPINS + spin) * TURNS
            for turn, values in enumerate((imag, real, -imag, -real, imag)):
                blocks_ref[start + turn] = values
    for gamma in range(out_ref.shape[1] // 2):
        places = [numbers_ref[first + gamma * SPINS + spin] for spin in range(SPINS)]
        out_ref[:, 2 * gamma, :] = sum(blocks_ref[place + 1] for place in places)
        out_ref[:, 2 * gamma + 1, :] = sum(blocks_ref[place] for place in places)


def finish(mine, theirs, left, right, numbers, first, factor):
    eig = mine.shape[0]
    rows = left.shape[0] // SPINS
    gammas = (numbers.shape[0] - first) // SPINS
    return pl.pallas_call(
        functools.partial(finish_body, factor, first),
        in_specs=[smem(), vmem(), vmem(), vmem(), vmem()],
        out_specs=vmem(),
        out_shape=jax.ShapeDtypeStruct((rows, 2 * gammas, eig), jnp.float32),
        scratch_shapes=[
            pltpu.VMEM((2 * eig, 2 * eig), jnp.bfloat16),
            pltpu.VMEM((2 * eig, 2 * eig), jnp.bfloat16),
            pltpu.VMEM((SPINS * SPINS * TURNS, rows, eig), jnp.float32),
        ],
        name="finish",
    )(scalars(numbers), resident(mine), resident(theirs), resident(left), resident(right))


def finish_plain(total, chosen, gamma_columns, gamma_phases, factor):
    eig = total.shape[0]
    precise = functools.partial(jnp.einsum, precision=lax.Precision.HIGHEST)
    rows = eig // lax.axis_size("space")
    start = lax.axis_index("space") * rows
    left = lax.dynamic_slice_in_dim(chosen[0], start, rows, axis=3).astype(jnp.float32)
    right = chosen[1].astype(jnp.float32)
    real, imag = total[:, :eig], total[:, eig:]
    front_real = precise("sla,lm->sam", left[:, 0], real) + precise("sla,lm->sam", left[:, 1], imag)
    front_imag = precise("sla,lm->sam", left[:, 0], imag) - precise("sla,lm->sam", left[:, 1], real)
    block_real = precise("sam,tmb->astb", front_real, right[:, 0]) - precise(
        "sam,tmb->astb", front_imag, right[:, 1]
    )
    block_imag = precise("sam,tmb->astb", front_real, right[:, 1]) + precise(
        "sam,tmb->astb", front_imag, right[:, 0]
    )
    matches = (gamma_columns[:, :, None] == jnp.arange(SPINS)[None, None, :]).astype(jnp.float32)
    along = (gamma_phases == 0).astype(jnp.float32) - (gamma_phases == 2).astype(jnp.float32)
    across = (gamma_phases == 1).astype(jnp.float32) - (gamma_phases == 3).astype(jnp.float32)
    along = matches * along[:, :, None]
    across = matches * across[:, :, None]
    out_real = precise("gst,astb->agb", along, block_real) - precise("gst,astb->agb", across, block_imag)
    out_imag = precise("gst,astb->agb", across, block_real) + precise("gst,astb->agb", along, block_imag)
    return factor * jnp.stack([out_real, out_imag], axis=2).reshape(rows, -1, eig)


def swap(values, distance, ranks):
    return lax.ppermute(values, "space", [(rank, rank ^ distance) for rank in range(ranks)])


def gather_slots(sent, kept, ranks):
    pairs = SPINS * 2
    pieces = [sent, kept]
    shards = [(0, 0, 0)]
    columns = {(0, relative): (1, index) for index, relative in enumerate(KEPT_OWNERS)}
    for distance in SLOT_DISTANCES:
        if distance == SLOT_DISTANCES[0]:
            held = sent
            moved = [(0, relative) for relative in SENT_OWNERS]
        else:
            moved = [key for key in columns if key[1] & distance]
            held = jnp.concatenate(
                [pieces[piece][first : first + pairs] for _, piece, first in shards]
                + [pieces[piece][index][None] for piece, index in (columns.pop(key) for key in moved)],
                axis=0,
            )
        pieces.append(swap(held, distance, ranks))
        arrived = len(pieces) - 1
        shards += [
            (source ^ distance, arrived, pairs * count) for count, (source, _, _) in enumerate(shards)
        ]
        for count, (source, owner) in enumerate(moved):
            columns[(source ^ distance, owner ^ distance)] = (arrived, pairs * len(shards) // 2 + count)
    plan = tuple(
        (source, piece, first) + columns[(source, 0)] for source, piece, first in shards
    )
    left, right = arrange(pieces, plan)
    return left, right


def on_device(eigvecs, perambulator, momenta, source_slots, gamma_columns, gamma_phases):
    local_sites = eigvecs.shape[1]
    eig_count = eigvecs.shape[4]
    ranks = lax.axis_size("space")
    total_sites = local_sites * ranks
    extent_x = total_sites // (LY * LZ)
    factor = 1.0 / math.sqrt(12.0 * total_sites)
    part_rows = perambulator.shape[4]
    rows_by_part = eigvecs.reshape(local_sites * COLORS * 2, eig_count)
    tiled = ranks == 8 and part_rows % 16 == 0 and part_rows * ranks == eig_count
    if tiled:
        sent, kept, rows_by_part, numbers = load(
            perambulator, source_slots, rows_by_part, momenta, gamma_columns, gamma_phases
        )
        left, right = gather_slots(sent, kept, ranks)
    else:
        chosen = lax.all_gather(
            jnp.take(perambulator[0], source_slots, axis=0), "space", axis=3, tiled=True
        )
        numbers = momenta.reshape(-1)
    results = []
    for index in range(momenta.shape[0]):
        total, narrow = overlap(rows_by_part, numbers, index, extent_x)
        if tiled:
            for distance in SUM_DISTANCES[:2]:
                received = swap(narrow, distance, ranks)
                total = total + received.astype(jnp.float32)
                narrow = total.astype(jnp.bfloat16)
            received = swap(narrow, SUM_DISTANCES[2], ranks)
            rows = finish(total, received, left, right, numbers, momenta.size, factor)
        else:
            total = lax.psum(total, "space")
            rows = finish_plain(total, chosen, gamma_columns, gamma_phases, factor)
        results.append(rows.reshape(rows.shape[0], gamma_columns.shape[0], 2, eig_count))
    return jnp.stack(results, axis=1)[None]


def solution(mesh):
    in_specs = (
        P(("cfg", "tm"), "space", None, None, None),
        P(("cfg", "tm"), None, None, None, "space", None),
        P(),
        P(),
        P(),
        P(),
    )
    out_specs = P(("cfg", "tm"), "space", None, None, None, None)
    return jax.shard_map(
        on_device, mesh=mesh, in_specs=in_specs, out_specs=out_specs, check_vma=False
    )
```

```python
import functools
import math

import jax
import jax.numpy as jnp
from jax import lax
from jax.experimental import pallas as pl
from jax.experimental.pallas import tpu as pltpu
from jax.sharding import PartitionSpec as P

LY = 48
LZ = 48
SPINS = 4
COLORS = 3
TURNS = 5
SLOT_DISTANCES = (2, 4, 1)
SUM_DISTANCES = (1, 2, 4)
KEPT_OWNERS = [e for e in range(8) if not e & SLOT_DISTANCES[0]]
SENT_OWNERS = [e for e in range(8) if e & SLOT_DISTANCES[0]]


def vmem():
    return pl.BlockSpec(memory_space=pltpu.VMEM)


def resident(array):
    return pltpu.with_memory_space_constraint(array, pltpu.VMEM)


def scalars(array):
    return pltpu.with_memory_space_constraint(array, pltpu.SMEM)


def smem():
    return pl.BlockSpec(memory_space=pltpu.SMEM)


def dot(left, right, left_dim=1, right_dim=0):
    return lax.dot_general(
        left, right, (((left_dim,), (right_dim,)), ((), ())), preferred_element_type=jnp.float32
    )


def split(values):
    high = values.astype(jnp.bfloat16)
    return high, (values - high.astype(jnp.float32)).astype(jnp.bfloat16)


def wrapped(product, length):
    return product - length * jnp.floor(product * (1.0 / length) + 0.5 / length)


def load_body(slots_hbm, momenta_hbm, columns_hbm, phases_hbm, source_ref, vectors_ref,
              sent_ref, kept_ref, loaded_ref, numbers_ref,
              stored_ref, turned_ref, slots_ref, momenta_ref, columns_ref, phases_ref, sems):
    pairs = SPINS * 2
    part_rows, eig = source_ref.shape[-2:]
    kept = kept_ref.shape[0]
    copies = [
        pltpu.make_async_copy(slots_hbm, slots_ref, sems.at[0]),
        pltpu.make_async_copy(source_ref.at[0], stored_ref, sems.at[1]),
        pltpu.make_async_copy(vectors_ref, loaded_ref, sems.at[2]),
        pltpu.make_async_copy(momenta_hbm, momenta_ref, sems.at[3]),
        pltpu.make_async_copy(columns_hbm, columns_ref, sems.at[4]),
        pltpu.make_async_copy(phases_hbm, phases_ref, sems.at[5]),
    ]
    for copy in copies:
        copy.start()
    copies[0].wait()
    copies[1].wait()
    sent_ref[pl.ds(0, pairs)] = stored_ref[slots_ref[1]]
    own = lax.axis_index("space")
    turned_ref[...] = stored_ref[slots_ref[0]].reshape(pairs * part_rows, eig).T
    for relative in range(2 * kept):
        start = pl.multiple_of((own ^ relative) * part_rows, part_rows)
        block = turned_ref[pl.ds(start, part_rows), :]
        if relative in KEPT_OWNERS:
            kept_ref[KEPT_OWNERS.index(relative)] = block
        else:
            sent_ref[pairs + SENT_OWNERS.index(relative)] = block
    for copy in copies[3:]:
        copy.wait()
    count, axes = momenta_ref.shape
    for index in range(count):
        for axis in range(axes):
            numbers_ref[index * axes + axis] = momenta_ref[index, axis]
    for gamma in range(columns_ref.shape[1]):
        for spin in range(SPINS):
            place = (columns_ref[spin, gamma] * SPINS + spin) * TURNS + phases_ref[spin, gamma]
            numbers_ref[count * axes + gamma * SPINS + spin] = place
    copies[2].wait()


def load(perambulator, source_slots, rows_by_part, momenta, gamma_columns, gamma_phases):
    _, slots, spins, parts, part_rows, eig = perambulator.shape
    pairs = spins * parts
    kept = eig // part_rows // 2
    kind = perambulator.dtype
    return pl.pallas_call(
        load_body,
        in_specs=[pl.BlockSpec(memory_space=pl.ANY)] * 6,
        out_specs=[vmem(), vmem(), vmem(), smem()],
        out_shape=[
            pltpu.VMEM((pairs + kept, part_rows, eig), kind),
            pltpu.VMEM((kept, part_rows, eig), kind),
            pltpu.VMEM(rows_by_part.shape, rows_by_part.dtype),
            pltpu.SMEM((momenta.size + gamma_columns.size,), jnp.int32),
        ],
        scratch_shapes=[
            pltpu.VMEM((slots, pairs, part_rows, eig), kind),
            pltpu.VMEM((eig, pairs * part_rows), kind),
            pltpu.SMEM(source_slots.shape, jnp.int32),
            pltpu.SMEM(momenta.shape, jnp.int32),
            pltpu.SMEM(gamma_columns.shape[::-1], jnp.int32),
            pltpu.SMEM(gamma_phases.shape[::-1], jnp.int32),
            pltpu.SemaphoreType.DMA((6,)),
        ],
        name="load",
    )(
        source_slots,
        momenta,
        gamma_columns.T,
        gamma_phases.T,
        perambulator.reshape(1, slots, pairs, part_rows, eig),
        rows_by_part,
    )


def overlap_body(extent_x, first, numbers_ref, vectors_ref, out_ref, narrow_ref, wide_ref, left_ref, both_ref):
    rows = left_ref.shape[0]
    eig = vectors_ref.shape[1]
    per_block = LZ * COLORS
    blocks = rows // per_block
    first_block = lax.axis_index("space") * blocks
    mom_x = numbers_ref[first + 0].astype(jnp.float32)
    mom_y = numbers_ref[first + 1].astype(jnp.float32)
    mom_z = numbers_ref[first + 2].astype(jnp.float32)
    wide_ref[...] = vectors_ref[...].astype(jnp.float32)
    row_ids = lax.broadcasted_iota(jnp.int32, (per_block, eig), 0).astype(jnp.float32)
    coord_z = jnp.floor((row_ids + 0.5) * (1.0 / COLORS))
    angle_z = (2.0 * math.pi / LZ) * wrapped(mom_z * coord_z, LZ)
    cos_z = jnp.cos(angle_z)
    sin_z = jnp.sin(angle_z)
    padded = -(-blocks // 8) * 8
    block_ids = (lax.broadcasted_iota(jnp.int32, (padded, eig), 0) + first_block).astype(jnp.float32)
    coord_x = jnp.floor((block_ids + 0.5) * (1.0 / LY))
    coord_y = block_ids - LY * coord_x
    angle_b = 2.0 * math.pi * (
        wrapped(mom_x * coord_x, extent_x) / extent_x + wrapped(mom_y * coord_y, LY) / LY
    )
    cos_b = jnp.cos(angle_b)
    sin_b = jnp.sin(angle_b)
    for block in range(blocks):
        own = pl.ds(block * per_block, per_block)
        real = wide_ref[pl.ds(2 * block * per_block, per_block, stride=2), :]
        imag = wide_ref[pl.ds(2 * block * per_block + 1, per_block, stride=2), :]
        left_ref[own, :eig] = real.astype(jnp.bfloat16)
        left_ref[own, eig:] = imag.astype(jnp.bfloat16)
        cos_own = cos_b[block : block + 1, :]
        sin_own = sin_b[block : block + 1, :]
        cosine = cos_own * cos_z - sin_own * sin_z
        sine = sin_own * cos_z + cos_own * sin_z
        wave_real = cosine * real - sine * imag
        wave_imag = sine * real + cosine * imag
        for part, wave in ((0, wave_real), (1, wave_imag)):
            high, low = split(wave)
            lanes = slice(part * eig, (part + 1) * eig)
            both_ref[own, lanes] = high
            both_ref[own, slice(lanes.start + 2 * eig, lanes.stop + 2 * eig)] = low
    left = left_ref[...]
    product = dot(left, both_ref[...], 0, 0)
    product = product[:, : 2 * eig] + product[:, 2 * eig :]
    out_ref[:, :eig] = product[:eig, :eig] + product[eig:, eig:]
    out_ref[:, eig:] = product[:eig, eig:] - product[eig:, :eig]
    narrow_ref[...] = out_ref[...].astype(jnp.bfloat16)


def overlap(rows_by_part, numbers, index, extent_x):
    rows = rows_by_part.shape[0] // 2
    eig = rows_by_part.shape[1]
    return pl.pallas_call(
        functools.partial(overlap_body, extent_x, 3 * index),
        in_specs=[smem(), vmem()],
        out_specs=[vmem(), vmem()],
        out_shape=[
            pltpu.VMEM((eig, 2 * eig), jnp.float32),
            pltpu.VMEM((eig, 2 * eig), jnp.bfloat16),
        ],
        scratch_shapes=[
            pltpu.VMEM((2 * rows, eig), jnp.float32),
            pltpu.VMEM((rows, 2 * eig), jnp.bfloat16),
            pltpu.VMEM((rows, 4 * eig), jnp.bfloat16),
        ],
        cost_estimate=pl.CostEstimate(
            flops=8 * rows * eig * eig * 2, bytes_accessed=4 * rows * eig, transcendentals=0
        ),
        name="overlap",
    )(scalars(numbers), resident(rows_by_part))


def arrange_body(plan, *refs):
    pieces = refs[:-2]
    left_ref, right_ref = refs[-2:]
    pairs = SPINS * 2
    own = lax.axis_index("space")
    part_rows, eig = pieces[0].shape[1:]
    lane_groups = lax.broadcasted_iota(jnp.int32, (part_rows, eig), 1) // part_rows
    rows = [jnp.zeros((part_rows, eig), jnp.float32) for _ in range(pairs)]
    for relative, right_piece, right_start, left_piece, left_index in plan:
        group = own ^ relative
        start = pl.multiple_of(group * part_rows, part_rows)
        for spin in range(SPINS):
            real = pieces[right_piece][right_start + 2 * spin]
            imag = pieces[right_piece][right_start + 2 * spin + 1]
            right_ref[spin, pl.ds(start, part_rows), :eig] = real
            right_ref[spin, pl.ds(start, part_rows), eig:] = imag
            right_ref[spin, pl.ds(eig + start, part_rows), :eig] = -imag
            right_ref[spin, pl.ds(eig + start, part_rows), eig:] = real
        block = pieces[left_piece][left_index].astype(jnp.float32)
        inside = lane_groups == group
        for pair in range(pairs):
            shift = lax.rem((group - pair + pairs) * part_rows, eig)
            rows[pair] = jnp.where(inside, pltpu.roll(block, shift, 1), rows[pair])
    for pair in range(pairs):
        spin, part = pair // 2, pair % 2
        left_ref[pl.ds((part * SPINS + spin) * part_rows, part_rows), :] = rows[pair].astype(jnp.bfloat16)


def arrange(pieces, plan):
    part_rows, eig = pieces[0].shape[1:]
    return pl.pallas_call(
        functools.partial(arrange_body, plan),
        in_specs=[vmem()] * len(pieces),
        out_specs=[vmem(), vmem()],
        out_shape=[
            pltpu.VMEM((2 * SPINS * part_rows, eig), jnp.bfloat16),
            pltpu.VMEM((SPINS, 2 * eig, 2 * eig), jnp.bfloat16),
        ],
        name="arrange",
    )(*[resident(piece) for piece in pieces])


def from_left(left, right):
    eig = right.shape[1] // 2
    product = dot(left, right)
    half = product.shape[0] // 2
    return jnp.concatenate(
        [
            product[:half, :eig] + product[half:, eig:],
            product[:half, eig:] - product[half:, :eig],
        ],
        axis=1,
    )


def finish_body(factor, first, numbers_ref, front_ref, theirs_ref, left_ref, right_ref, out_ref, blocks_ref):
    eig = theirs_ref.shape[0]
    rows = out_ref.shape[0]
    front = factor * (front_ref[...] + from_left(left_ref[...], theirs_ref[...]))
    high, low = split(front)
    both = jnp.concatenate([high, low], axis=0)
    for column in range(SPINS):
        product = dot(both, right_ref[column])
        product = product[: SPINS * rows] + product[SPINS * rows :]
        for spin in range(SPINS):
            real = product[spin * rows : (spin + 1) * rows, :eig]
            imag = product[spin * rows : (spin + 1) * rows, eig:]
            start = (column * SPINS + spin) * TURNS
            for turn, values in enumerate((imag, real, -imag, -real, imag)):
                blocks_ref[start + turn] = values
    for gamma in range(out_ref.shape[1] // 2):
        places = [numbers_ref[first + gamma * SPINS + spin] for spin in range(SPINS)]
        out_ref[:, 2 * gamma, :] = sum(blocks_ref[place + 1] for place in places)
        out_ref[:, 2 * gamma + 1, :] = sum(blocks_ref[place] for place in places)


def finish(front, theirs, left, right, numbers, first, factor):
    eig = theirs.shape[0]
    rows = left.shape[0] // SPINS // 2
    gammas = (numbers.shape[0] - first) // SPINS
    return pl.pallas_call(
        functools.partial(finish_body, factor, first),
        in_specs=[smem(), vmem(), vmem(), vmem(), vmem()],
        out_specs=vmem(),
        out_shape=jax.ShapeDtypeStruct((rows, 2 * gammas, eig), jnp.float32),
        scratch_shapes=[
            pltpu.VMEM((SPINS * SPINS * TURNS, rows, eig), jnp.float32),
        ],
        name="finish",
    )(scalars(numbers), resident(front), resident(theirs), resident(left), resident(right))


def begin_finish_body(left_ref, mine_ref, front_ref):
    left = left_ref[...]
    high, low = split(mine_ref[...])
    front_ref[...] = from_left(left, high) + from_left(left, low)


def begin_finish(left, mine):
    return pl.pallas_call(
        begin_finish_body,
        in_specs=[vmem(), vmem()],
        out_specs=vmem(),
        out_shape=pltpu.VMEM((left.shape[0] // 2, mine.shape[1]), jnp.float32),
        name="begin_finish",
    )(resident(left), resident(mine))


def finish_plain(total, chosen, gamma_columns, gamma_phases, factor):
    eig = total.shape[0]
    precise = functools.partial(jnp.einsum, precision=lax.Precision.HIGHEST)
    rows = eig // lax.axis_size("space")
    start = lax.axis_index("space") * rows
    left = lax.dynamic_slice_in_dim(chosen[0], start, rows, axis=3).astype(jnp.float32)
    right = chosen[1].astype(jnp.float32)
    real, imag = total[:, :eig], total[:, eig:]
    front_real = precise("sla,lm->sam", left[:, 0], real) + precise("sla,lm->sam", left[:, 1], imag)
    front_imag = precise("sla,lm->sam", left[:, 0], imag) - precise("sla,lm->sam", left[:, 1], real)
    block_real = precise("sam,tmb->astb", front_real, right[:, 0]) - precise(
        "sam,tmb->astb", front_imag, right[:, 1]
    )
    block_imag = precise("sam,tmb->astb", front_real, right[:, 1]) + precise(
        "sam,tmb->astb", front_imag, right[:, 0]
    )
    matches = (gamma_columns[:, :, None] == jnp.arange(SPINS)[None, None, :]).astype(jnp.float32)
    along = (gamma_phases == 0).astype(jnp.float32) - (gamma_phases == 2).astype(jnp.float32)
    across = (gamma_phases == 1).astype(jnp.float32) - (gamma_phases == 3).astype(jnp.float32)
    along = matches * along[:, :, None]
    across = matches * across[:, :, None]
    out_real = precise("gst,astb->agb", along, block_real) - precise("gst,astb->agb", across, block_imag)
    out_imag = precise("gst,astb->agb", across, block_real) + precise("gst,astb->agb", along, block_imag)
    return factor * jnp.stack([out_real, out_imag], axis=2).reshape(rows, -1, eig)


def swap(values, distance, ranks):
    return lax.ppermute(values, "space", [(rank, rank ^ distance) for rank in range(ranks)])


def gather_slots(sent, kept, ranks):
    pairs = SPINS * 2
    pieces = [sent, kept]
    shards = [(0, 0, 0)]
    columns = {(0, relative): (1, index) for index, relative in enumerate(KEPT_OWNERS)}
    for distance in SLOT_DISTANCES:
        if distance == SLOT_DISTANCES[0]:
            held = sent
            moved = [(0, relative) for relative in SENT_OWNERS]
        else:
            moved = [key for key in columns if key[1] & distance]
            held = jnp.concatenate(
                [pieces[piece][first : first + pairs] for _, piece, first in shards]
                + [pieces[piece][index][None] for piece, index in (columns.pop(key) for key in moved)],
                axis=0,
            )
        pieces.append(swap(held, distance, ranks))
        arrived = len(pieces) - 1
        shards += [
            (source ^ distance, arrived, pairs * count) for count, (source, _, _) in enumerate(shards)
        ]
        for count, (source, owner) in enumerate(moved):
            columns[(source ^ distance, owner ^ distance)] = (arrived, pairs * len(shards) // 2 + count)
    plan = tuple(
        (source, piece, first) + columns[(source, 0)] for source, piece, first in shards
    )
    left, right = arrange(pieces, plan)
    return left, right


def on_device(eigvecs, perambulator, momenta, source_slots, gamma_columns, gamma_phases):
    local_sites = eigvecs.shape[1]
    eig_count = eigvecs.shape[4]
    ranks = lax.axis_size("space")
    total_sites = local_sites * ranks
    extent_x = total_sites // (LY * LZ)
    factor = 1.0 / math.sqrt(12.0 * total_sites)
    part_rows = perambulator.shape[4]
    rows_by_part = eigvecs.reshape(local_sites * COLORS * 2, eig_count)
    tiled = ranks == 8 and part_rows % 16 == 0 and part_rows * ranks == eig_count
    if tiled:
        sent, kept, rows_by_part, numbers = load(
            perambulator, source_slots, rows_by_part, momenta, gamma_columns, gamma_phases
        )
        left, right = gather_slots(sent, kept, ranks)
    else:
        chosen = lax.all_gather(
            jnp.take(perambulator[0], source_slots, axis=0), "space", axis=3, tiled=True
        )
        numbers = momenta.reshape(-1)
    results = []
    for index in range(momenta.shape[0]):
        total, narrow = overlap(rows_by_part, numbers, index, extent_x)
        if tiled:
            for distance in SUM_DISTANCES[:2]:
                received = swap(narrow, distance, ranks)
                total = total + received.astype(jnp.float32)
                narrow = total.astype(jnp.bfloat16)
            received = swap(narrow, SUM_DISTANCES[2], ranks)
            rows = finish(begin_finish(left, total), received, left, right, numbers, momenta.size, factor)
        else:
            total = lax.psum(total, "space")
            rows = finish_plain(total, chosen, gamma_columns, gamma_phases, factor)
        results.append(rows.reshape(rows.shape[0], gamma_columns.shape[0], 2, eig_count))
    return jnp.stack(results, axis=1)[None]


def solution(mesh):
    in_specs = (
        P(("cfg", "tm"), "space", None, None, None),
        P(("cfg", "tm"), None, None, None, "space", None),
        P(),
        P(),
        P(),
        P(),
    )
    out_specs = P(("cfg", "tm"), "space", None, None, None, None)
    return jax.shard_map(
        on_device, mesh=mesh, in_specs=in_specs, out_specs=out_specs, check_vma=False
    )
```

```python
import functools
import math

import jax
import jax.numpy as jnp
from jax import lax
from jax.experimental import pallas as pl
from jax.experimental.pallas import tpu as pltpu
from jax.sharding import PartitionSpec as P

LY = 48
LZ = 48
SPINS = 4
COLORS = 3
TURNS = 5
SLOT_DISTANCES = (2, 4, 1)
SUM_DISTANCES = (1, 2, 4)
KEPT_OWNERS = [e for e in range(8) if not e & SLOT_DISTANCES[0]]
SENT_OWNERS = [e for e in range(8) if e & SLOT_DISTANCES[0]]


def vmem():
    return pl.BlockSpec(memory_space=pltpu.VMEM)


def resident(array):
    return pltpu.with_memory_space_constraint(array, pltpu.VMEM)


def scalars(array):
    return pltpu.with_memory_space_constraint(array, pltpu.SMEM)


def smem():
    return pl.BlockSpec(memory_space=pltpu.SMEM)


def dot(left, right, left_dim=1, right_dim=0):
    return lax.dot_general(
        left, right, (((left_dim,), (right_dim,)), ((), ())), preferred_element_type=jnp.float32
    )


def split(values):
    high = values.astype(jnp.bfloat16)
    return high, (values - high.astype(jnp.float32)).astype(jnp.bfloat16)


def wrapped(product, length):
    return product - length * jnp.floor(product * (1.0 / length) + 0.5 / length)


def turned(turns):
    quarters = jnp.floor(4.0 * turns + 0.5)
    angle = (2.0 * math.pi) * (turns - 0.25 * quarters)
    square = angle * angle
    cosine = jnp.ones_like(angle)
    sine = jnp.ones_like(angle)
    for power in (10, 8, 6, 4, 2):
        cosine = 1.0 - square * cosine * (1.0 / (power * (power - 1)))
        sine = 1.0 - square * sine * (1.0 / (power * (power + 1)))
    sine = angle * sine
    quarters = quarters - 4.0 * jnp.floor(0.25 * quarters)
    odd = (quarters == 1.0) | (quarters == 3.0)
    swapped_cosine = jnp.where(odd, sine, cosine)
    swapped_sine = jnp.where(odd, cosine, sine)
    return (
        jnp.where((quarters == 1.0) | (quarters == 2.0), -swapped_cosine, swapped_cosine),
        jnp.where(quarters >= 2.0, -swapped_sine, swapped_sine),
    )


def load_body(slots_hbm, momenta_hbm, columns_hbm, phases_hbm, source_ref, vectors_ref,
              sent_ref, kept_ref, loaded_ref, numbers_ref,
              stored_ref, turned_ref, slots_ref, momenta_ref, columns_ref, phases_ref, sems):
    pairs = SPINS * 2
    part_rows, eig = source_ref.shape[-2:]
    kept = kept_ref.shape[0]
    copies = [
        pltpu.make_async_copy(slots_hbm, slots_ref, sems.at[0]),
        pltpu.make_async_copy(source_ref.at[0], stored_ref, sems.at[1]),
        pltpu.make_async_copy(vectors_ref, loaded_ref, sems.at[2]),
        pltpu.make_async_copy(momenta_hbm, momenta_ref, sems.at[3]),
        pltpu.make_async_copy(columns_hbm, columns_ref, sems.at[4]),
        pltpu.make_async_copy(phases_hbm, phases_ref, sems.at[5]),
    ]
    for copy in copies:
        copy.start()
    copies[0].wait()
    copies[1].wait()
    sent_ref[pl.ds(0, pairs)] = stored_ref[slots_ref[1]]
    own = lax.axis_index("space")
    turned_ref[...] = stored_ref[slots_ref[0]].reshape(pairs * part_rows, eig).T
    for relative in range(2 * kept):
        start = pl.multiple_of((own ^ relative) * part_rows, part_rows)
        block = turned_ref[pl.ds(start, part_rows), :]
        if relative in KEPT_OWNERS:
            kept_ref[KEPT_OWNERS.index(relative)] = block
        else:
            sent_ref[pairs + SENT_OWNERS.index(relative)] = block
    for copy in copies[3:]:
        copy.wait()
    count, axes = momenta_ref.shape
    for index in range(count):
        for axis in range(axes):
            numbers_ref[index * axes + axis] = momenta_ref[index, axis]
    for gamma in range(columns_ref.shape[1]):
        for spin in range(SPINS):
            place = (columns_ref[spin, gamma] * SPINS + spin) * TURNS + phases_ref[spin, gamma]
            numbers_ref[count * axes + gamma * SPINS + spin] = place
    copies[2].wait()


def load(perambulator, source_slots, rows_by_part, momenta, gamma_columns, gamma_phases):
    _, slots, spins, parts, part_rows, eig = perambulator.shape
    pairs = spins * parts
    kept = eig // part_rows // 2
    kind = perambulator.dtype
    return pl.pallas_call(
        load_body,
        in_specs=[pl.BlockSpec(memory_space=pl.ANY)] * 6,
        out_specs=[vmem(), vmem(), vmem(), smem()],
        out_shape=[
            pltpu.VMEM((pairs + kept, part_rows, eig), kind),
            pltpu.VMEM((kept, part_rows, eig), kind),
            pltpu.VMEM(rows_by_part.shape, rows_by_part.dtype),
            pltpu.SMEM((momenta.size + gamma_columns.size,), jnp.int32),
        ],
        scratch_shapes=[
            pltpu.VMEM((slots, pairs, part_rows, eig), kind),
            pltpu.VMEM((eig, pairs * part_rows), kind),
            pltpu.SMEM(source_slots.shape, jnp.int32),
            pltpu.SMEM(momenta.shape, jnp.int32),
            pltpu.SMEM(gamma_columns.shape[::-1], jnp.int32),
            pltpu.SMEM(gamma_phases.shape[::-1], jnp.int32),
            pltpu.SemaphoreType.DMA((6,)),
        ],
        name="load",
    )(
        source_slots,
        momenta,
        gamma_columns.T,
        gamma_phases.T,
        perambulator.reshape(1, slots, pairs, part_rows, eig),
        rows_by_part,
    )


def overlap_body(extent_x, first, numbers_ref, vectors_ref, out_ref, narrow_ref, wide_ref, left_ref, both_ref):
    rows = left_ref.shape[0]
    eig = vectors_ref.shape[1]
    per_block = LZ * COLORS
    blocks = rows // per_block
    first_block = lax.axis_index("space") * blocks
    mom_x = numbers_ref[first + 0].astype(jnp.float32)
    mom_y = numbers_ref[first + 1].astype(jnp.float32)
    mom_z = numbers_ref[first + 2].astype(jnp.float32)
    wide_ref[...] = vectors_ref[...].astype(jnp.float32)
    row_ids = lax.broadcasted_iota(jnp.int32, (per_block, eig), 0).astype(jnp.float32)
    coord_z = jnp.floor((row_ids + 0.5) * (1.0 / COLORS))
    cos_z, sin_z = turned(wrapped(mom_z * coord_z, LZ) * (1.0 / LZ))
    padded = -(-blocks // 8) * 8
    block_ids = (lax.broadcasted_iota(jnp.int32, (padded, eig), 0) + first_block).astype(jnp.float32)
    coord_x = jnp.floor((block_ids + 0.5) * (1.0 / LY))
    coord_y = block_ids - LY * coord_x
    cos_b, sin_b = turned(
        wrapped(mom_x * coord_x, extent_x) * (1.0 / extent_x) + wrapped(mom_y * coord_y, LY) * (1.0 / LY)
    )
    for block in range(blocks):
        own = pl.ds(block * per_block, per_block)
        real = wide_ref[pl.ds(2 * block * per_block, per_block, stride=2), :]
        imag = wide_ref[pl.ds(2 * block * per_block + 1, per_block, stride=2), :]
        left_ref[own, :eig] = real.astype(jnp.bfloat16)
        left_ref[own, eig:] = imag.astype(jnp.bfloat16)
        cos_own = cos_b[block : block + 1, :]
        sin_own = sin_b[block : block + 1, :]
        cosine = cos_own * cos_z - sin_own * sin_z
        sine = sin_own * cos_z + cos_own * sin_z
        wave_real = cosine * real - sine * imag
        wave_imag = sine * real + cosine * imag
        for part, wave in ((0, wave_real), (1, wave_imag)):
            high, low = split(wave)
            lanes = slice(part * eig, (part + 1) * eig)
            both_ref[own, lanes] = high
            both_ref[own, slice(lanes.start + 2 * eig, lanes.stop + 2 * eig)] = low
    left = left_ref[...]
    product = dot(left, both_ref[...], 0, 0)
    product = product[:, : 2 * eig] + product[:, 2 * eig :]
    out_ref[:, :eig] = product[:eig, :eig] + product[eig:, eig:]
    out_ref[:, eig:] = product[:eig, eig:] - product[eig:, :eig]
    narrow_ref[...] = out_ref[...].astype(jnp.bfloat16)


def overlap(rows_by_part, numbers, index, extent_x):
    rows = rows_by_part.shape[0] // 2
    eig = rows_by_part.shape[1]
    return pl.pallas_call(
        functools.partial(overlap_body, extent_x, 3 * index),
        in_specs=[smem(), vmem()],
        out_specs=[vmem(), vmem()],
        out_shape=[
            pltpu.VMEM((eig, 2 * eig), jnp.float32),
            pltpu.VMEM((eig, 2 * eig), jnp.bfloat16),
        ],
        scratch_shapes=[
            pltpu.VMEM((2 * rows, eig), jnp.float32),
            pltpu.VMEM((rows, 2 * eig), jnp.bfloat16),
            pltpu.VMEM((rows, 4 * eig), jnp.bfloat16),
        ],
        cost_estimate=pl.CostEstimate(
            flops=8 * rows * eig * eig * 2, bytes_accessed=4 * rows * eig, transcendentals=0
        ),
        name="overlap",
    )(scalars(numbers), resident(rows_by_part))


def arrange_body(plan, *refs):
    pieces = refs[:-2]
    left_ref, right_ref = refs[-2:]
    pairs = SPINS * 2
    own = lax.axis_index("space")
    part_rows, eig = pieces[0].shape[1:]
    lane_groups = lax.broadcasted_iota(jnp.int32, (part_rows, eig), 1) // part_rows
    rows = [jnp.zeros((part_rows, eig), jnp.float32) for _ in range(pairs)]
    for relative, right_piece, right_start, left_piece, left_index in plan:
        group = own ^ relative
        start = pl.multiple_of(group * part_rows, part_rows)
        for spin in range(SPINS):
            real = pieces[right_piece][right_start + 2 * spin]
            imag = pieces[right_piece][right_start + 2 * spin + 1]
            right_ref[spin, pl.ds(start, part_rows), :eig] = real
            right_ref[spin, pl.ds(start, part_rows), eig:] = imag
            right_ref[spin, pl.ds(eig + start, part_rows), :eig] = -imag
            right_ref[spin, pl.ds(eig + start, part_rows), eig:] = real
        block = pieces[left_piece][left_index].astype(jnp.float32)
        inside = lane_groups == group
        for pair in range(pairs):
            shift = lax.rem((group - pair + pairs) * part_rows, eig)
            rows[pair] = jnp.where(inside, pltpu.roll(block, shift, 1), rows[pair])
    for pair in range(pairs):
        spin, part = pair // 2, pair % 2
        left_ref[pl.ds((part * SPINS + spin) * part_rows, part_rows), :] = rows[pair].astype(jnp.bfloat16)


def arrange(pieces, plan):
    part_rows, eig = pieces[0].shape[1:]
    return pl.pallas_call(
        functools.partial(arrange_body, plan),
        in_specs=[vmem()] * len(pieces),
        out_specs=[vmem(), vmem()],
        out_shape=[
            pltpu.VMEM((2 * SPINS * part_rows, eig), jnp.bfloat16),
            pltpu.VMEM((SPINS, 2 * eig, 2 * eig), jnp.bfloat16),
        ],
        name="arrange",
    )(*[resident(piece) for piece in pieces])


def from_left(left, right):
    eig = right.shape[1] // 2
    product = dot(left, right)
    half = product.shape[0] // 2
    return jnp.concatenate(
        [
            product[:half, :eig] + product[half:, eig:],
            product[:half, eig:] - product[half:, :eig],
        ],
        axis=1,
    )


def finish_body(factor, first, numbers_ref, front_ref, theirs_ref, left_ref, right_ref, out_ref, blocks_ref):
    eig = theirs_ref.shape[0]
    rows = out_ref.shape[0]
    front = factor * (front_ref[...] + from_left(left_ref[...], theirs_ref[...]))
    high, low = split(front)
    both = jnp.concatenate([high, low], axis=0)
    for column in range(SPINS):
        product = dot(both, right_ref[column])
        product = product[: SPINS * rows] + product[SPINS * rows :]
        for spin in range(SPINS):
            real = product[spin * rows : (spin + 1) * rows, :eig]
            imag = product[spin * rows : (spin + 1) * rows, eig:]
            start = (column * SPINS + spin) * TURNS
            for turn, values in enumerate((imag, real, -imag, -real, imag)):
                blocks_ref[start + turn] = values
    for gamma in range(out_ref.shape[1] // 2):
        places = [numbers_ref[first + gamma * SPINS + spin] for spin in range(SPINS)]
        out_ref[:, 2 * gamma, :] = sum(blocks_ref[place + 1] for place in places)
        out_ref[:, 2 * gamma + 1, :] = sum(blocks_ref[place] for place in places)


def finish(front, theirs, left, right, numbers, first, factor):
    eig = theirs.shape[0]
    rows = left.shape[0] // SPINS // 2
    gammas = (numbers.shape[0] - first) // SPINS
    return pl.pallas_call(
        functools.partial(finish_body, factor, first),
        in_specs=[smem(), vmem(), vmem(), vmem(), vmem()],
        out_specs=vmem(),
        out_shape=jax.ShapeDtypeStruct((rows, 2 * gammas, eig), jnp.float32),
        scratch_shapes=[
            pltpu.VMEM((SPINS * SPINS * TURNS, rows, eig), jnp.float32),
        ],
        name="finish",
    )(scalars(numbers), resident(front), resident(theirs), resident(left), resident(right))


def begin_finish_body(left_ref, mine_ref, front_ref):
    left = left_ref[...]
    high, low = split(mine_ref[...])
    front_ref[...] = from_left(left, high) + from_left(left, low)


def begin_finish(left, mine):
    return pl.pallas_call(
        begin_finish_body,
        in_specs=[vmem(), vmem()],
        out_specs=vmem(),
        out_shape=pltpu.VMEM((left.shape[0] // 2, mine.shape[1]), jnp.float32),
        name="begin_finish",
    )(resident(left), resident(mine))


def finish_plain(total, chosen, gamma_columns, gamma_phases, factor):
    eig = total.shape[0]
    precise = functools.partial(jnp.einsum, precision=lax.Precision.HIGHEST)
    rows = eig // lax.axis_size("space")
    start = lax.axis_index("space") * rows
    left = lax.dynamic_slice_in_dim(chosen[0], start, rows, axis=3).astype(jnp.float32)
    right = chosen[1].astype(jnp.float32)
    real, imag = total[:, :eig], total[:, eig:]
    front_real = precise("sla,lm->sam", left[:, 0], real) + precise("sla,lm->sam", left[:, 1], imag)
    front_imag = precise("sla,lm->sam", left[:, 0], imag) - precise("sla,lm->sam", left[:, 1], real)
    block_real = precise("sam,tmb->astb", front_real, right[:, 0]) - precise(
        "sam,tmb->astb", front_imag, right[:, 1]
    )
    block_imag = precise("sam,tmb->astb", front_real, right[:, 1]) + precise(
        "sam,tmb->astb", front_imag, right[:, 0]
    )
    matches = (gamma_columns[:, :, None] == jnp.arange(SPINS)[None, None, :]).astype(jnp.float32)
    along = (gamma_phases == 0).astype(jnp.float32) - (gamma_phases == 2).astype(jnp.float32)
    across = (gamma_phases == 1).astype(jnp.float32) - (gamma_phases == 3).astype(jnp.float32)
    along = matches * along[:, :, None]
    across = matches * across[:, :, None]
    out_real = precise("gst,astb->agb", along, block_real) - precise("gst,astb->agb", across, block_imag)
    out_imag = precise("gst,astb->agb", across, block_real) + precise("gst,astb->agb", along, block_imag)
    return factor * jnp.stack([out_real, out_imag], axis=2).reshape(rows, -1, eig)


def swap(values, distance, ranks):
    return lax.ppermute(values, "space", [(rank, rank ^ distance) for rank in range(ranks)])


def gather_slots(sent, kept, ranks):
    pairs = SPINS * 2
    pieces = [sent, kept]
    shards = [(0, 0, 0)]
    columns = {(0, relative): (1, index) for index, relative in enumerate(KEPT_OWNERS)}
    for distance in SLOT_DISTANCES:
        if distance == SLOT_DISTANCES[0]:
            held = sent
            moved = [(0, relative) for relative in SENT_OWNERS]
        else:
            moved = [key for key in columns if key[1] & distance]
            held = jnp.concatenate(
                [pieces[piece][first : first + pairs] for _, piece, first in shards]
                + [pieces[piece][index][None] for piece, index in (columns.pop(key) for key in moved)],
                axis=0,
            )
        pieces.append(swap(held, distance, ranks))
        arrived = len(pieces) - 1
        shards += [
            (source ^ distance, arrived, pairs * count) for count, (source, _, _) in enumerate(shards)
        ]
        for count, (source, owner) in enumerate(moved):
            columns[(source ^ distance, owner ^ distance)] = (arrived, pairs * len(shards) // 2 + count)
    plan = tuple(
        (source, piece, first) + columns[(source, 0)] for source, piece, first in shards
    )
    left, right = arrange(pieces, plan)
    return left, right


def on_device(eigvecs, perambulator, momenta, source_slots, gamma_columns, gamma_phases):
    local_sites = eigvecs.shape[1]
    eig_count = eigvecs.shape[4]
    ranks = lax.axis_size("space")
    total_sites = local_sites * ranks
    extent_x = total_sites // (LY * LZ)
    factor = 1.0 / math.sqrt(12.0 * total_sites)
    part_rows = perambulator.shape[4]
    rows_by_part = eigvecs.reshape(local_sites * COLORS * 2, eig_count)
    tiled = ranks == 8 and part_rows % 16 == 0 and part_rows * ranks == eig_count
    if tiled:
        sent, kept, rows_by_part, numbers = load(
            perambulator, source_slots, rows_by_part, momenta, gamma_columns, gamma_phases
        )
        left, right = gather_slots(sent, kept, ranks)
    else:
        chosen = lax.all_gather(
            jnp.take(perambulator[0], source_slots, axis=0), "space", axis=3, tiled=True
        )
        numbers = momenta.reshape(-1)
    results = []
    for index in range(momenta.shape[0]):
        total, narrow = overlap(rows_by_part, numbers, index, extent_x)
        if tiled:
            for distance in SUM_DISTANCES[:2]:
                received = swap(narrow, distance, ranks)
                total = total + received.astype(jnp.float32)
                narrow = total.astype(jnp.bfloat16)
            received = swap(narrow, SUM_DISTANCES[2], ranks)
            rows = finish(begin_finish(left, total), received, left, right, numbers, momenta.size, factor)
        else:
            total = lax.psum(total, "space")
            rows = finish_plain(total, chosen, gamma_columns, gamma_phases, factor)
        results.append(rows.reshape(rows.shape[0], gamma_columns.shape[0], 2, eig_count))
    return jnp.stack(results, axis=1)[None]


def solution(mesh):
    in_specs = (
        P(("cfg", "tm"), "space", None, None, None),
        P(("cfg", "tm"), None, None, None, "space", None),
        P(),
        P(),
        P(),
        P(),
    )
    out_specs = P(("cfg", "tm"), "space", None, None, None, None)
    return jax.shard_map(
        on_device, mesh=mesh, in_specs=in_specs, out_specs=out_specs, check_vma=False
    )
```

```python
import functools
import math

import jax
import jax.numpy as jnp
from jax import lax
from jax.experimental import pallas as pl
from jax.experimental.pallas import tpu as pltpu
from jax.sharding import PartitionSpec as P

LY = 48
LZ = 48
SPINS = 4
COLORS = 3
TURNS = 5
SLOT_DISTANCES = (2, 4, 1)
SUM_DISTANCES = (1, 2, 4)
KEPT_OWNERS = [e for e in range(8) if not e & SLOT_DISTANCES[0]]
SENT_OWNERS = [e for e in range(8) if e & SLOT_DISTANCES[0]]


def vmem():
    return pl.BlockSpec(memory_space=pltpu.VMEM)


def resident(array):
    return pltpu.with_memory_space_constraint(array, pltpu.VMEM)


def scalars(array):
    return pltpu.with_memory_space_constraint(array, pltpu.SMEM)


def smem():
    return pl.BlockSpec(memory_space=pltpu.SMEM)


def dot(left, right, left_dim=1, right_dim=0):
    return lax.dot_general(
        left, right, (((left_dim,), (right_dim,)), ((), ())), preferred_element_type=jnp.float32
    )


def split(values):
    high = values.astype(jnp.bfloat16)
    return high, (values - high.astype(jnp.float32)).astype(jnp.bfloat16)


def wrapped(product, length):
    return product - length * jnp.floor(product * (1.0 / length) + 0.5 / length)


def turned(turns):
    quarters = jnp.floor(4.0 * turns + 0.5)
    angle = (2.0 * math.pi) * (turns - 0.25 * quarters)
    square = angle * angle
    cosine = jnp.ones_like(angle)
    sine = jnp.ones_like(angle)
    for power in (10, 8, 6, 4, 2):
        cosine = 1.0 - square * cosine * (1.0 / (power * (power - 1)))
        sine = 1.0 - square * sine * (1.0 / (power * (power + 1)))
    sine = angle * sine
    quarters = quarters - 4.0 * jnp.floor(0.25 * quarters)
    odd = (quarters == 1.0) | (quarters == 3.0)
    swapped_cosine = jnp.where(odd, sine, cosine)
    swapped_sine = jnp.where(odd, cosine, sine)
    return (
        jnp.where((quarters == 1.0) | (quarters == 2.0), -swapped_cosine, swapped_cosine),
        jnp.where(quarters >= 2.0, -swapped_sine, swapped_sine),
    )


def load_body(slots_hbm, momenta_hbm, columns_hbm, phases_hbm, source_ref, vectors_ref,
              sent_ref, kept_ref, loaded_ref, numbers_ref,
              stored_ref, turned_ref, slots_ref, momenta_ref, columns_ref, phases_ref, sems):
    pairs = SPINS * 2
    part_rows, eig = source_ref.shape[-2:]
    kept = kept_ref.shape[0]
    copies = [
        pltpu.make_async_copy(slots_hbm, slots_ref, sems.at[0]),
        pltpu.make_async_copy(source_ref.at[0], stored_ref, sems.at[1]),
        pltpu.make_async_copy(vectors_ref, loaded_ref, sems.at[2]),
        pltpu.make_async_copy(momenta_hbm, momenta_ref, sems.at[3]),
        pltpu.make_async_copy(columns_hbm, columns_ref, sems.at[4]),
        pltpu.make_async_copy(phases_hbm, phases_ref, sems.at[5]),
    ]
    for copy in copies:
        copy.start()
    for copy in copies[3:]:
        copy.wait()
    count, axes = momenta_ref.shape
    for index in range(count):
        for axis in range(axes):
            numbers_ref[index * axes + axis] = momenta_ref[index, axis]
    for gamma in range(columns_ref.shape[1]):
        for spin in range(SPINS):
            place = (columns_ref[spin, gamma] * SPINS + spin) * TURNS + phases_ref[spin, gamma]
            numbers_ref[count * axes + gamma * SPINS + spin] = place
    copies[0].wait()
    copies[1].wait()
    sent_ref[pl.ds(0, pairs)] = stored_ref[slots_ref[1]]
    own = lax.axis_index("space")
    turned_ref[...] = stored_ref[slots_ref[0]].reshape(pairs * part_rows, eig).T
    for relative in range(2 * kept):
        start = pl.multiple_of((own ^ relative) * part_rows, part_rows)
        block = turned_ref[pl.ds(start, part_rows), :]
        if relative in KEPT_OWNERS:
            kept_ref[KEPT_OWNERS.index(relative)] = block
        else:
            sent_ref[pairs + SENT_OWNERS.index(relative)] = block
    copies[2].wait()


def load(perambulator, source_slots, rows_by_part, momenta, gamma_columns, gamma_phases):
    _, slots, spins, parts, part_rows, eig = perambulator.shape
    pairs = spins * parts
    kept = eig // part_rows // 2
    kind = perambulator.dtype
    return pl.pallas_call(
        load_body,
        in_specs=[pl.BlockSpec(memory_space=pl.ANY)] * 6,
        out_specs=[vmem(), vmem(), vmem(), smem()],
        out_shape=[
            pltpu.VMEM((pairs + kept, part_rows, eig), kind),
            pltpu.VMEM((kept, part_rows, eig), kind),
            pltpu.VMEM(rows_by_part.shape, rows_by_part.dtype),
            pltpu.SMEM((momenta.size + gamma_columns.size,), jnp.int32),
        ],
        scratch_shapes=[
            pltpu.VMEM((slots, pairs, part_rows, eig), kind),
            pltpu.VMEM((eig, pairs * part_rows), kind),
            pltpu.SMEM(source_slots.shape, jnp.int32),
            pltpu.SMEM(momenta.shape, jnp.int32),
            pltpu.SMEM(gamma_columns.shape[::-1], jnp.int32),
            pltpu.SMEM(gamma_phases.shape[::-1], jnp.int32),
            pltpu.SemaphoreType.DMA((6,)),
        ],
        name="load",
    )(
        source_slots,
        momenta,
        gamma_columns.T,
        gamma_phases.T,
        perambulator.reshape(1, slots, pairs, part_rows, eig),
        rows_by_part,
    )


def overlap_body(extent_x, first, numbers_ref, vectors_ref, out_ref, narrow_ref, wide_ref, left_ref, both_ref):
    rows = left_ref.shape[0]
    eig = vectors_ref.shape[1]
    per_block = LZ * COLORS
    blocks = rows // per_block
    first_block = lax.axis_index("space") * blocks
    mom_x = numbers_ref[first + 0].astype(jnp.float32)
    mom_y = numbers_ref[first + 1].astype(jnp.float32)
    mom_z = numbers_ref[first + 2].astype(jnp.float32)
    wide_ref[...] = vectors_ref[...].astype(jnp.float32)
    row_ids = lax.broadcasted_iota(jnp.int32, (per_block, eig), 0).astype(jnp.float32)
    coord_z = jnp.floor((row_ids + 0.5) * (1.0 / COLORS))
    cos_z, sin_z = turned(wrapped(mom_z * coord_z, LZ) * (1.0 / LZ))
    padded = -(-blocks // 8) * 8
    block_ids = (lax.broadcasted_iota(jnp.int32, (padded, eig), 0) + first_block).astype(jnp.float32)
    coord_x = jnp.floor((block_ids + 0.5) * (1.0 / LY))
    coord_y = block_ids - LY * coord_x
    cos_b, sin_b = turned(
        wrapped(mom_x * coord_x, extent_x) * (1.0 / extent_x) + wrapped(mom_y * coord_y, LY) * (1.0 / LY)
    )
    for block in range(blocks):
        own = pl.ds(block * per_block, per_block)
        real = wide_ref[pl.ds(2 * block * per_block, per_block, stride=2), :]
        imag = wide_ref[pl.ds(2 * block * per_block + 1, per_block, stride=2), :]
        left_ref[own, :eig] = real.astype(jnp.bfloat16)
        left_ref[own, eig:] = imag.astype(jnp.bfloat16)
        cos_own = cos_b[block : block + 1, :]
        sin_own = sin_b[block : block + 1, :]
        cosine = cos_own * cos_z - sin_own * sin_z
        sine = sin_own * cos_z + cos_own * sin_z
        wave_real = cosine * real - sine * imag
        wave_imag = sine * real + cosine * imag
        for part, wave in ((0, wave_real), (1, wave_imag)):
            high, low = split(wave)
            lanes = slice(part * eig, (part + 1) * eig)
            both_ref[own, lanes] = high
            both_ref[own, slice(lanes.start + 2 * eig, lanes.stop + 2 * eig)] = low
    left = left_ref[...]
    product = dot(left, both_ref[...], 0, 0)
    product = product[:, : 2 * eig] + product[:, 2 * eig :]
    out_ref[:, :eig] = product[:eig, :eig] + product[eig:, eig:]
    out_ref[:, eig:] = product[:eig, eig:] - product[eig:, :eig]
    narrow_ref[...] = out_ref[...].astype(jnp.bfloat16)


def overlap(rows_by_part, numbers, index, extent_x):
    rows = rows_by_part.shape[0] // 2
    eig = rows_by_part.shape[1]
    return pl.pallas_call(
        functools.partial(overlap_body, extent_x, 3 * index),
        in_specs=[smem(), vmem()],
        out_specs=[vmem(), vmem()],
        out_shape=[
            pltpu.VMEM((eig, 2 * eig), jnp.float32),
            pltpu.VMEM((eig, 2 * eig), jnp.bfloat16),
        ],
        scratch_shapes=[
            pltpu.VMEM((2 * rows, eig), jnp.float32),
            pltpu.VMEM((rows, 2 * eig), jnp.bfloat16),
            pltpu.VMEM((rows, 4 * eig), jnp.bfloat16),
        ],
        cost_estimate=pl.CostEstimate(
            flops=8 * rows * eig * eig * 2, bytes_accessed=4 * rows * eig, transcendentals=0
        ),
        name="overlap",
    )(scalars(numbers), resident(rows_by_part))


def arrange_body(plan, *refs):
    pieces = refs[:-2]
    left_ref, right_ref = refs[-2:]
    pairs = SPINS * 2
    own = lax.axis_index("space")
    part_rows, eig = pieces[0].shape[1:]
    lane_groups = lax.broadcasted_iota(jnp.int32, (part_rows, eig), 1) // part_rows
    rows = [jnp.zeros((part_rows, eig), jnp.float32) for _ in range(pairs)]
    for relative, right_piece, right_start, left_piece, left_index in plan:
        group = own ^ relative
        start = pl.multiple_of(group * part_rows, part_rows)
        for spin in range(SPINS):
            real = pieces[right_piece][right_start + 2 * spin]
            imag = pieces[right_piece][right_start + 2 * spin + 1]
            right_ref[spin, pl.ds(start, part_rows), :eig] = real
            right_ref[spin, pl.ds(start, part_rows), eig:] = imag
            right_ref[spin, pl.ds(eig + start, part_rows), :eig] = -imag
            right_ref[spin, pl.ds(eig + start, part_rows), eig:] = real
        block = pieces[left_piece][left_index].astype(jnp.float32)
        inside = lane_groups == group
        for pair in range(pairs):
            shift = lax.rem((group - pair + pairs) * part_rows, eig)
            rows[pair] = jnp.where(inside, pltpu.roll(block, shift, 1), rows[pair])
    for pair in range(pairs):
        spin, part = pair // 2, pair % 2
        left_ref[pl.ds((part * SPINS + spin) * part_rows, part_rows), :] = rows[pair].astype(jnp.bfloat16)


def arrange(pieces, plan):
    part_rows, eig = pieces[0].shape[1:]
    return pl.pallas_call(
        functools.partial(arrange_body, plan),
        in_specs=[vmem()] * len(pieces),
        out_specs=[vmem(), vmem()],
        out_shape=[
            pltpu.VMEM((2 * SPINS * part_rows, eig), jnp.bfloat16),
            pltpu.VMEM((SPINS, 2 * eig, 2 * eig), jnp.bfloat16),
        ],
        name="arrange",
    )(*[resident(piece) for piece in pieces])


def from_left(left, right):
    eig = right.shape[1] // 2
    product = dot(left, right)
    half = product.shape[0] // 2
    return jnp.concatenate(
        [
            product[:half, :eig] + product[half:, eig:],
            product[:half, eig:] - product[half:, :eig],
        ],
        axis=1,
    )


def finish_body(factor, first, numbers_ref, front_ref, theirs_ref, left_ref, right_ref, out_ref, blocks_ref):
    eig = theirs_ref.shape[0]
    rows = out_ref.shape[0]
    front = factor * (front_ref[...] + from_left(left_ref[...], theirs_ref[...]))
    high, low = split(front)
    both = jnp.concatenate([high, low], axis=0)
    for column in range(SPINS):
        product = dot(both, right_ref[column])
        product = product[: SPINS * rows] + product[SPINS * rows :]
        for spin in range(SPINS):
            real = product[spin * rows : (spin + 1) * rows, :eig]
            imag = product[spin * rows : (spin + 1) * rows, eig:]
            start = (column * SPINS + spin) * TURNS
            for turn, values in enumerate((imag, real, -imag, -real, imag)):
                blocks_ref[start + turn] = values
    for gamma in range(out_ref.shape[1] // 2):
        places = [numbers_ref[first + gamma * SPINS + spin] for spin in range(SPINS)]
        out_ref[:, 2 * gamma, :] = sum(blocks_ref[place + 1] for place in places)
        out_ref[:, 2 * gamma + 1, :] = sum(blocks_ref[place] for place in places)


def finish(front, theirs, left, right, numbers, first, factor):
    eig = theirs.shape[0]
    rows = left.shape[0] // SPINS // 2
    gammas = (numbers.shape[0] - first) // SPINS
    return pl.pallas_call(
        functools.partial(finish_body, factor, first),
        in_specs=[smem(), vmem(), vmem(), vmem(), vmem()],
        out_specs=vmem(),
        out_shape=jax.ShapeDtypeStruct((rows, 2 * gammas, eig), jnp.float32),
        scratch_shapes=[
            pltpu.VMEM((SPINS * SPINS * TURNS, rows, eig), jnp.float32),
        ],
        name="finish",
    )(scalars(numbers), resident(front), resident(theirs), resident(left), resident(right))


def begin_finish_body(left_ref, mine_ref, front_ref):
    left = left_ref[...]
    high, low = split(mine_ref[...])
    front_ref[...] = from_left(left, high) + from_left(left, low)


def begin_finish(left, mine):
    return pl.pallas_call(
        begin_finish_body,
        in_specs=[vmem(), vmem()],
        out_specs=vmem(),
        out_shape=pltpu.VMEM((left.shape[0] // 2, mine.shape[1]), jnp.float32),
        name="begin_finish",
    )(resident(left), resident(mine))


def finish_plain(total, chosen, gamma_columns, gamma_phases, factor):
    eig = total.shape[0]
    precise = functools.partial(jnp.einsum, precision=lax.Precision.HIGHEST)
    rows = eig // lax.axis_size("space")
    start = lax.axis_index("space") * rows
    left = lax.dynamic_slice_in_dim(chosen[0], start, rows, axis=3).astype(jnp.float32)
    right = chosen[1].astype(jnp.float32)
    real, imag = total[:, :eig], total[:, eig:]
    front_real = precise("sla,lm->sam", left[:, 0], real) + precise("sla,lm->sam", left[:, 1], imag)
    front_imag = precise("sla,lm->sam", left[:, 0], imag) - precise("sla,lm->sam", left[:, 1], real)
    block_real = precise("sam,tmb->astb", front_real, right[:, 0]) - precise(
        "sam,tmb->astb", front_imag, right[:, 1]
    )
    block_imag = precise("sam,tmb->astb", front_real, right[:, 1]) + precise(
        "sam,tmb->astb", front_imag, right[:, 0]
    )
    matches = (gamma_columns[:, :, None] == jnp.arange(SPINS)[None, None, :]).astype(jnp.float32)
    along = (gamma_phases == 0).astype(jnp.float32) - (gamma_phases == 2).astype(jnp.float32)
    across = (gamma_phases == 1).astype(jnp.float32) - (gamma_phases == 3).astype(jnp.float32)
    along = matches * along[:, :, None]
    across = matches * across[:, :, None]
    out_real = precise("gst,astb->agb", along, block_real) - precise("gst,astb->agb", across, block_imag)
    out_imag = precise("gst,astb->agb", across, block_real) + precise("gst,astb->agb", along, block_imag)
    return factor * jnp.stack([out_real, out_imag], axis=2).reshape(rows, -1, eig)


def swap(values, distance, ranks):
    return lax.ppermute(values, "space", [(rank, rank ^ distance) for rank in range(ranks)])


def gather_slots(sent, kept, ranks):
    pairs = SPINS * 2
    pieces = [sent, kept]
    shards = [(0, 0, 0)]
    columns = {(0, relative): (1, index) for index, relative in enumerate(KEPT_OWNERS)}
    for distance in SLOT_DISTANCES:
        if distance == SLOT_DISTANCES[0]:
            held = sent
            moved = [(0, relative) for relative in SENT_OWNERS]
        else:
            moved = [key for key in columns if key[1] & distance]
            held = jnp.concatenate(
                [pieces[piece][first : first + pairs] for _, piece, first in shards]
                + [pieces[piece][index][None] for piece, index in (columns.pop(key) for key in moved)],
                axis=0,
            )
        pieces.append(swap(held, distance, ranks))
        arrived = len(pieces) - 1
        shards += [
            (source ^ distance, arrived, pairs * count) for count, (source, _, _) in enumerate(shards)
        ]
        for count, (source, owner) in enumerate(moved):
            columns[(source ^ distance, owner ^ distance)] = (arrived, pairs * len(shards) // 2 + count)
    plan = tuple(
        (source, piece, first) + columns[(source, 0)] for source, piece, first in shards
    )
    left, right = arrange(pieces, plan)
    return left, right


def on_device(eigvecs, perambulator, momenta, source_slots, gamma_columns, gamma_phases):
    local_sites = eigvecs.shape[1]
    eig_count = eigvecs.shape[4]
    ranks = lax.axis_size("space")
    total_sites = local_sites * ranks
    extent_x = total_sites // (LY * LZ)
    factor = 1.0 / math.sqrt(12.0 * total_sites)
    part_rows = perambulator.shape[4]
    rows_by_part = eigvecs.reshape(local_sites * COLORS * 2, eig_count)
    tiled = ranks == 8 and part_rows % 16 == 0 and part_rows * ranks == eig_count
    if tiled:
        sent, kept, rows_by_part, numbers = load(
            perambulator, source_slots, rows_by_part, momenta, gamma_columns, gamma_phases
        )
        left, right = gather_slots(sent, kept, ranks)
    else:
        chosen = lax.all_gather(
            jnp.take(perambulator[0], source_slots, axis=0), "space", axis=3, tiled=True
        )
        numbers = momenta.reshape(-1)
    results = []
    for index in range(momenta.shape[0]):
        total, narrow = overlap(rows_by_part, numbers, index, extent_x)
        if tiled:
            for distance in SUM_DISTANCES[:2]:
                received = swap(narrow, distance, ranks)
                total = total + received.astype(jnp.float32)
                narrow = total.astype(jnp.bfloat16)
            received = swap(narrow, SUM_DISTANCES[2], ranks)
            rows = finish(begin_finish(left, total), received, left, right, numbers, momenta.size, factor)
        else:
            total = lax.psum(total, "space")
            rows = finish_plain(total, chosen, gamma_columns, gamma_phases, factor)
        results.append(rows.reshape(rows.shape[0], gamma_columns.shape[0], 2, eig_count))
    return jnp.stack(results, axis=1)[None]


def solution(mesh):
    in_specs = (
        P(("cfg", "tm"), "space", None, None, None),
        P(("cfg", "tm"), None, None, None, "space", None),
        P(),
        P(),
        P(),
        P(),
    )
    out_specs = P(("cfg", "tm"), "space", None, None, None, None)
    return jax.shard_map(
        on_device, mesh=mesh, in_specs=in_specs, out_specs=out_specs, check_vma=False
    )
```
